16 devices in a mesh: depth: 2 (over z), col: 2 (over y), row: 4 (over x, core).
Axes of the slice: x: 2, y: 2, z: 2, core: 2. Of those that a mesh axis runs over, the one named last changes fastest.
Arguments:
- tokens: bfloat16 [16384, 1024], P(('depth', 'row'), 'col')
- w_up: bfloat16 [1024, 4096], P('row', 'col')
- w_down: bfloat16 [4096, 1024], P('row', 'col')
- grad_out: bfloat16 [16384, 1024], P(('depth', 'row'), 'col')
Outputs:
- output 1: bfloat16 [16384, 1024], P(('depth', 'row'), 'col')
- output 2: bfloat16 [16384, 1024], P(('depth', 'row'), 'col')
- output 3: float32 [1024, 4096], P('row', 'col')
- output 4: float32 [4096, 1024], P('row', 'col')
All inputs are finite; a program needn't handle non-finite values.
Results may differ from the reference program's by a relative error of at most 0.001.
Values are sent between devices in bfloat16 or wider.
A program may use at most 1 GiB of HBM per device.

```python
import math
import jax
import jax.numpy as jnp
from jax import lax

TOKENS_DEV = 2048
HIDDEN = 1024
FFN_WIDTH = 4096
BLOCKS = 8
TOKENS = TOKENS_DEV * BLOCKS
INV_ROOT_TWO = 1.0 / math.sqrt(2.0)
INV_ROOT_TAU = 1.0 / math.sqrt(2.0 * math.pi)


def setup_inputs(seed: int = 0) -> dict:
    base_key = jax.random.key(seed)
    key_tok, key_up, key_down, key_grad = jax.random.split(base_key, 4)
    tokens = jax.random.normal(key_tok, (TOKENS, HIDDEN), jnp.float32)
    w_up = jax.random.normal(key_up, (HIDDEN, FFN_WIDTH), jnp.float32) * (HIDDEN ** -0.5)
    w_down = jax.random.normal(key_down, (FFN_WIDTH, HIDDEN), jnp.float32) * (FFN_WIDTH ** -0.5)
    grad_out = jax.random.normal(key_grad, (TOKENS, HIDDEN), jnp.float32)
    return {"tokens": tokens.astype(jnp.bfloat16), "w_up": w_up.astype(jnp.bfloat16), "w_down": w_down.astype(jnp.bfloat16), "grad_out": grad_out.astype(jnp.bfloat16)}


def gelu_value(pre_act):
    return 0.5 * pre_act * (1.0 + lax.erf(pre_act * INV_ROOT_TWO))


def gelu_slope(pre_act):
    return 0.5 * (1.0 + lax.erf(pre_act * INV_ROOT_TWO)) + pre_act * jnp.exp(-0.5 * pre_act * pre_act) * INV_ROOT_TAU


def reference(tokens, w_up, w_down, grad_out):
    tok_blocks = tokens.reshape(BLOCKS, TOKENS_DEV, HIDDEN)
    grad_blocks = grad_out.reshape(BLOCKS, TOKENS_DEV, HIDDEN)

    def one_block(acc_pair, blk_pair):
        acc_up, acc_down = acc_pair
        tok_blk, grad_blk = blk_pair
        pre_act = jnp.dot(tok_blk, w_up, preferred_element_type=jnp.float32)
        hidden_act = gelu_value(pre_act).astype(jnp.bfloat16)
        out_blk = jnp.dot(hidden_act, w_down, preferred_element_type=jnp.float32).astype(jnp.bfloat16)
        grad_act = jnp.dot(grad_blk, w_down.T, preferred_element_type=jnp.float32)
        grad_pre = (grad_act * gelu_slope(pre_act)).astype(jnp.bfloat16)
        grad_tok = jnp.dot(grad_pre, w_up.T, preferred_element_type=jnp.float32).astype(jnp.bfloat16)
        acc_down = acc_down + jnp.dot(hidden_act.T, grad_blk, preferred_element_type=jnp.float32)
        acc_up = acc_up + jnp.dot(tok_blk.T, grad_pre, preferred_element_type=jnp.float32)
        return (acc_up, acc_down), (out_blk, grad_tok)

    start_acc = (jnp.zeros((HIDDEN, FFN_WIDTH), jnp.float32), jnp.zeros((FFN_WIDTH, HIDDEN), jnp.float32))
    (grad_w_up, grad_w_down), (out_blocks, grad_tok_blocks) = lax.scan(one_block, start_acc, (tok_blocks, grad_blocks))
    return (out_blocks.reshape(TOKENS, HIDDEN), grad_tok_blocks.reshape(TOKENS, HIDDEN), grad_w_up, grad_w_down)
```

```python
import math
import jax
import jax.numpy as jnp
from jax import lax
from jax.sharding import PartitionSpec as P

INV_ROOT_TWO = 1.0 / math.sqrt(2.0)
INV_ROOT_TAU = 1.0 / math.sqrt(2.0 * math.pi)


def solution(mesh):
    act_spec = P(("depth", "row"), "col")
    wgt_spec = P("row", "col")
    n_row = mesh.shape["row"]
    bf16, f32 = jnp.bfloat16, jnp.float32

    def over_x(v):
        return lax.ppermute(v, "row", [(i, i ^ 2) for i in range(n_row)])

    def over_core(v):
        return lax.ppermute(v, "row", [(i, i ^ 1) for i in range(n_row)])

    def over_y(v):
        return lax.ppermute(v, "col", [(0, 1), (1, 0)])

    def over_z(v):
        return lax.ppermute(v, "depth", [(0, 1), (1, 0)])

    def cat_abs(first, own, other, axis):
        return jnp.where(first, jnp.concatenate([own, other], axis), jnp.concatenate([other, own], axis))

    def dot(a, b, ca, cb):
        return lax.dot_general(a, b, (((ca,), (cb,)), ((), ())), preferred_element_type=f32)

    def block(tok, up, down, grad):
        z = lax.axis_index("depth")
        y = lax.axis_index("col")
        r = lax.axis_index("row")
        x, c = r // 2, r % 2
        eq = x == y
        th = tok.shape[0] // 2
        hh = tok.shape[1]
        fb = up.shape[1] // 2

        def take_tokens(v):
            keep = lax.dynamic_slice_in_dim(v, y * th, th, 0)
            send = lax.dynamic_slice_in_dim(v, (1 - y) * th, th, 0)
            mine = jnp.concatenate([keep, over_y(send)], 1)
            return jnp.concatenate([mine, over_core(mine)], 0)

        up_keep = lax.dynamic_slice_in_dim(up, c * fb, fb, 1)
        up_send = lax.dynamic_slice_in_dim(up, (1 - c) * fb, fb, 1)
        xs = take_tokens(tok)
        up_own = cat_abs(c == 0, up_keep, over_core(up_send), 0)
        up_x = over_x(up_own)
        up_b0 = jnp.where(eq, jnp.concatenate([up_own, up_x], 0), jnp.concatenate([up_x, up_own], 0))
        up_in = over_y(jnp.concatenate([up_own, up_x], 0))
        up_b1 = jnp.where(eq, jnp.concatenate([up_in[:hh], up_in[hh:]], 0), jnp.concatenate([up_in[hh:], up_in[:hh]], 0))
        w1 = [jnp.where(eq, up_b0, up_b1), jnp.where(eq, up_b1, up_b0)]
        gs = take_tokens(grad)
        down_y = over_y(lax.optimization_barrier((down, xs))[0])
        w2_0 = jnp.concatenate([down, down_y], 1)
        w2 = [w2_0, over_x(w2_0)]

        x_keep = jnp.where(eq, xs[:, :hh], xs[:, hh:])
        x_send = jnp.where(eq, xs[:, hh:], xs[:, :hh])

        d2, d1k, d1s, d2z = {}, {}, {}, {}
        y_part = dx_part = None
        for k in (1, 0):
            u = dot(xs, w1[k], 1, 0)
            cdf = 0.5 * (1.0 + lax.erf(u * INV_ROOT_TWO))
            act = (u * cdf).astype(bf16)
            slope = cdf + u * jnp.exp(-0.5 * u * u) * INV_ROOT_TAU
            d2[k] = dot(act, gs, 0, 0)
            d2z[k] = over_z(lax.dynamic_slice_in_dim(d2[k], (1 - z) * hh, hh, 0))
            du = (dot(gs, w2[k], 1, 1) * slope).astype(bf16)
            d1s[k] = over_x(dot(x_send, du, 0, 0))
            d1k[k] = dot(x_keep, du, 0, 0)
            yp = dot(act, w2[k], 1, 0)
            y_part = yp if y_part is None else y_part + yp
            dp = dot(du, w1[k], 1, 1)
            dx_part = dp if dx_part is None else dx_part + dp

        def give_tokens(part):
            mine = (part[:th] + over_core(part[th:])).astype(bf16)
            return cat_abs(y == 0, mine[:, :hh], over_y(mine[:, hh:]), 0)

        half = [lax.dynamic_slice_in_dim(d2[k], z * hh, hh, 0) + d2z[k] for k in (0, 1)]
        s2 = half[0] + over_x(half[1])
        s2 = s2[:, :hh] + over_y(s2[:, hh:])
        g_down = cat_abs(z == 0, s2, over_z(s2), 0)
        s_0 = d1k[0] + d1s[1]
        s_1 = d1k[1] + d1s[0]
        s1 = jnp.where(eq, s_0, s_1) + over_y(jnp.where(eq, s_1, s_0))
        s1 = s1 + over_z(s1)
        rows = s1.shape[0] // 2
        keep = lax.dynamic_slice_in_dim(s1, c * rows, rows, 0)
        send = lax.dynamic_slice_in_dim(s1, (1 - c) * rows, rows, 0)
        g_up = cat_abs(c == 0, keep, over_core(send), 1)
        return give_tokens(y_part), give_tokens(dx_part), g_up, g_down

    return jax.shard_map(block, mesh=mesh, in_specs=(act_spec, wgt_spec, wgt_spec, act_spec),
                         out_specs=(act_spec, act_spec, wgt_spec, wgt_spec), check_vma=False)
```

```python
import math
import jax
import jax.numpy as jnp
from jax import lax
from jax.experimental import pallas as pl
from jax.experimental.pallas import tpu as pltpu
from jax.sharding import PartitionSpec as P

INV_ROOT_TWO = 1.0 / math.sqrt(2.0)
INV_ROOT_TAU = 1.0 / math.sqrt(2.0 * math.pi)
MESH = pl.DeviceIdType.MESH
BF16, F32 = jnp.bfloat16, jnp.float32

TOK, HID, FC, NCH = 2048, 1024, 256, 8
HALF, TILE = 512, 512
Z2, X1, X2, Y2, Y1, Z1, ZO, C1, CP, YO = 0, 8, 16, 20, 24, 28, 32, 36, 40, 42
WY1, WX1, WP, WF1, WY2, WX2, WF2, TY, TP, TF, NSEM = 44, 52, 60, 64, 68, 72, 76, 80, 82, 84, 86


def dot(a, b, ca, cb):
    return lax.dot_general(a, b, (((ca,), (cb,)), ((), ())), preferred_element_type=F32)


def kernel(x_in, g_in, up_in, down_in, y_out, dx_out, d1_out, d2_out, yl, dl, w1b, w2b,
           xs, gs, yacc, dxacc, d1, d2, zr2, xr1, xr2, yr2, yr1, zr1, w1s, w2s, stage,
           send, recv, loc, wsem, isem):
    z, y, r = lax.axis_index("depth"), lax.axis_index("col"), lax.axis_index("row")
    x, c = r // 2, r % 2
    dev_c, dev_x = (z, y, r + 1 - 2 * c), (z, y, (1 - x) * 2 + c)
    dev_y, dev_z = (z, 1 - y, r), (1 - z, y, r)
    dev_xc, dev_yc = (z, y, (1 - x) * 2 + 1 - c), (z, 1 - y, r + 1 - 2 * c)
    zrow = pl.ds(pl.multiple_of(z * 128, 128), 128)
    zoth = pl.ds(pl.multiple_of((1 - z) * 128, 128), 128)
    lo, hi = pl.ds(0, HALF), pl.ds(HALF, HALF)
    mine, theirs = pl.ds(0, TOK // 2), pl.ds(TOK // 2, TOK // 2)
    tok_rows = pl.ds(pl.multiple_of(y * (TOK // 2), TOK // 2), TOK // 2)
    oth_rows = pl.ds(pl.multiple_of((1 - y) * (TOK // 2), TOK // 2), TOK // 2)

    def rc2(ks, kr, src, dst, dev):
        return pltpu.make_async_remote_copy(src_ref=src, dst_ref=dst, send_sem=send.at[ks], recv_sem=recv.at[kr],
                                            device_id=dev, device_id_type=MESH)

    def rc(k, src, dst, dev):
        return rc2(k, k, src, dst, dev)

    barrier = pltpu.get_barrier_semaphore()
    for dev in (dev_c, dev_x, dev_y, dev_z, dev_xc, dev_yc):
        pl.semaphore_signal(barrier, inc=1, device_id=dev, device_id_type=MESH)
    pl.semaphore_wait(barrier, 6)

    def chunk(q):
        return pl.ds(pl.multiple_of(q * FC, FC), FC)

    def up_cols(core, s):
        return pl.ds(pl.multiple_of(core * HID + s * FC, FC), FC)

    def t_wy1(s, core, sender):
        dev = (z, 1 - y, x * 2 + core)
        return rc2(WY1 + 2 * s + core, WY1 + 2 * s + sender, up_in.at[:, up_cols(core, s)],
                   w1b.at[y, chunk(c), chunk(s)], dev)

    def t_wx1(s, core, sender):
        dev = (z, y, (1 - x) * 2 + core)
        return rc2(WX1 + 2 * s + core, WX1 + 2 * s + sender, up_in.at[:, up_cols(core, s)],
                   w1b.at[y, chunk(2 + c), chunk(s)], dev)

    def t_wp(s):
        return rc(WP + s, up_in.at[:, up_cols(1 - c, s)], w1b.at[y, chunk(c), chunk(s)], dev_c)

    def t_wf1(s):
        return rc(WF1 + s, w1b.at[1 - y, lo, chunk(s)], w1b.at[1 - y, hi, chunk(s)], dev_x)

    def t_wy2(s):
        return rc(WY2 + s, down_in.at[chunk(s), :], w2b.at[x, chunk(s), hi], dev_y)

    def t_wx2(s):
        return rc(WX2 + s, down_in.at[chunk(s), :], w2b.at[x, chunk(s), lo], dev_x)

    def t_wf2(s):
        return rc(WF2 + s, w2b.at[x, chunk(s), hi], w2b.at[x, chunk(s), hi], dev_x)

    def send_wy(s):
        for core in (0, 1):
            t_wy1(s, core, c).start()
        t_wy2(s).start()

    def send_wx(s):
        for core in (0, 1):
            t_wx1(s, core, c).start()
        t_wx2(s).start()
        t_wp(s).start()

    def forward_w(s):
        for core in (0, 1):
            t_wy1(s, core, core).wait_recv()
        t_wy2(s).wait_recv()
        t_wf1(s).start()
        t_wf2(s).start()

    def arrive_w(s):
        for core in (0, 1):
            t_wx1(s, core, core).wait_recv()
        t_wx2(s).wait_recv()
        t_wp(s).wait_recv()
        t_wf1(s).wait_recv()
        t_wf2(s).wait_recv()

    eq_off = pl.multiple_of(jnp.where(x == y, 0, HALF), HALF)
    ne_off = pl.multiple_of(jnp.where(x == y, HALF, 0), HALF)
    own_cols = (pl.ds(eq_off, HALF), lo)
    far_cols = (pl.ds(ne_off, HALF), hi)

    def t_ty(i):
        return rc(TY + i, (x_in, g_in)[i].at[oth_rows, :], (xs, gs)[i].at[mine, (own_cols[0], hi)[i]], dev_y)

    def t_tp(i):
        return rc(TP + i, (x_in, g_in)[i].at[tok_rows, :], (xs, gs)[i].at[theirs, own_cols[i]], dev_c)

    def t_tf(i):
        return rc(TF + i, (xs, gs)[i].at[mine, far_cols[i]], (xs, gs)[i].at[theirs, far_cols[i]], dev_c)

    def l_t(i):
        return pltpu.make_async_copy((x_in, g_in)[i].at[tok_rows, :], (xs, gs)[i].at[mine, own_cols[i]], isem.at[i])

    send_wy(0)
    send_wx(0)
    for i in (0, 1):
        t_ty(i).start()
        l_t(i).start()
        t_tp(i).start()
    send_wx(1)
    for s in (1, 2, 3):
        send_wy(s)

    def load_w(j, slot, start):
        s, b = j // 2, j % 2

        def go(src, dst, k):
            cp = pltpu.make_async_copy(src, dst, wsem.at[slot, k])
            cp.start() if start else cp.wait()
        v1, v2 = w1s.at[slot], w2s.at[slot]
        if start:
            @pl.when(b == y)
            def _():
                go(up_in.at[:, up_cols(c, s)], v1.at[chunk(c), :], 0)

            @pl.when(b != y)
            def _():
                go(w1b.at[b, chunk(c), chunk(s)], v1.at[chunk(c), :], 0)

            @pl.when(b == x)
            def _():
                go(down_in.at[chunk(s), :], v2.at[:, lo], 3)

            @pl.when(b != x)
            def _():
                go(w2b.at[b, chunk(s), lo], v2.at[:, lo], 3)
        else:
            go(up_in.at[:, up_cols(c, s)], v1.at[chunk(c), :], 0)
            go(down_in.at[chunk(s), :], v2.at[:, lo], 3)
        go(w1b.at[b, chunk(1 - c), chunk(s)], v1.at[chunk(1 - c), :], 1)
        go(w1b.at[b, hi, chunk(s)], v1.at[hi, :], 2)
        go(w2b.at[b, chunk(s), hi], v2.at[:, hi], 4)

    def zero(i, _):
        rows = pl.ds(pl.multiple_of(i * 64, 64), 64)
        yacc[rows, :] = jnp.zeros((64, HID), F32)
        dxacc[rows, :] = jnp.zeros((64, HID), F32)
        return 0
    lax.fori_loop(0, TOK // 64, zero, 0)
    forward_w(0)
    send_wx(2)
    send_wx(3)
    arrive_w(0)
    load_w(0, 0, True)
    for i in (0, 1):
        t_ty(i).wait_recv()
        t_tf(i).start()
        l_t(i).wait()
        t_tp(i).wait_recv()
    for i in (0, 1):
        t_tf(i).wait_recv()

    def t_z2(j):
        return rc(Z2 + j, d2.at[j, zoth, :], zr2.at[j], dev_z)

    def t_x1(j):
        return rc(X1 + j, d1.at[j, :, hi], xr1.at[j], dev_x)

    def t_x2(s):
        return rc(X2 + s, d2.at[2 * s + 1 - x, zrow, :], xr2.at[s], dev_x)

    def t_y1(s):
        return rc(Y1 + s, d1.at[2 * s + 1 - y, :, lo], yr1.at[s], dev_y)

    def t_y2(s):
        return rc(Y2 + s, d2.at[2 * s + x, zrow, hi], yr2.at[s], dev_y)

    def t_z1(s):
        return rc(Z1 + s, d1.at[2 * s + y, :, lo], zr1.at[s], dev_z)

    def o2_rows(s):
        return d2_out.at[pl.ds(pl.multiple_of(s * FC + z * 128, 128), 128), :]

    def o1_rows(s):
        return d1_out.at[pl.ds(pl.multiple_of(c * HID + s * FC, FC), FC), :]

    def cols_c(q):
        return pl.ds(pl.multiple_of(q * 256, 256), 256)

    def t_zo(s):
        return rc(ZO + s, yr2.at[s], o2_rows(s), dev_z)

    def t_zo_in(s):
        return rc(ZO + s, yr2.at[s], d2_out.at[pl.ds(pl.multiple_of(s * FC + (1 - z) * 128, 128), 128), :], dev_z)

    def l_o2(s):
        return pltpu.make_async_copy(yr2.at[s], o2_rows(s), loc.at[s])

    def t_c1(s):
        return rc(C1 + s, zr1.at[s, :, cols_c(1 - c)], o1_rows(s), dev_c)

    def l_o1(s):
        return pltpu.make_async_copy(zr1.at[s, :, cols_c(c)], o1_rows(s), loc.at[4 + s])

    def t_cp(i):
        return rc(CP + i, (yacc, dxacc)[i].at[theirs, :], (yl, dl)[i], dev_c)

    def compute(j):
        slot = j % 2

        load_w(j, slot, False)
        w1, w2 = w1s.at[slot], w2s.at[slot]

        def tile(t, _):
            rows = pl.ds(pl.multiple_of(t * TILE, TILE), TILE)

            @pl.when(jnp.logical_and(t == TOK // TILE - 1, j + 1 < NCH))
            def _():
                @pl.when(slot == 1)
                def _():
                    arrive_w((j + 1) // 2)
                load_w(j + 1, 1 - slot, True)
            xt, gt = xs[rows, :], gs[rows, :]
            u = dot(xt, w1[...], 1, 0)
            da = dot(gt, w2[...], 1, 1)
            cdf = 0.5 * (1.0 + lax.erf(u * INV_ROOT_TWO))
            act = (u * cdf).astype(BF16)
            du = (da * (cdf + u * jnp.exp(-0.5 * u * u) * INV_ROOT_TAU)).astype(BF16)
            yacc[rows, :] += dot(act, w2[...], 1, 0)
            dxacc[rows, :] += dot(du, w1[...], 1, 1)
            p2, p1 = dot(act, gt, 0, 0), dot(du, xt, 0, 0)

            @pl.when(t == 0)
            def _():
                d2[j] = p2
                d1[j] = p1

            @pl.when(t > 0)
            def _():
                d2[j] += p2
                d1[j] += p1
            return 0
        lax.fori_loop(0, TOK // TILE, tile, 0)
        t_z2(j).start()
        t_x1(j).start()

    def stage_b(j):
        t_z2(j).wait_recv()
        d2[j, zrow, :] += zr2[j]
        t_x1(j).wait_recv()
        d1[j, :, :HALF] += xr1[j]

    def stage_c(s):
        t_x2(s).start()
        t_y1(s).start()

    def stage_d(s):
        t_x2(s).wait_recv()
        d2[2 * s + x, zrow, :] += xr2[s]
        t_y2(s).start()
        t_y1(s).wait_recv()
        d1[2 * s + y, :, :HALF] += yr1[s]
        t_z1(s).start()

    def stage_e(s):
        t_y2(s).wait_recv()
        yr2[s] += d2[2 * s + x, zrow, :HALF]
        t_zo(s).start()
        l_o2(s).start()
        t_z1(s).wait_recv()
        zr1[s] += d1[2 * s + y, :, :HALF]
        t_c1(s).start()
        l_o1(s).start()

    def step(j, _):
        @pl.when(j < NCH)
        def _():
            compute(j)

        @pl.when(j < 3)
        def _():
            forward_w(j + 1)

        @pl.when(j == NCH - 1)
        def _():
            t_cp(0).start()
            t_cp(1).start()

        @pl.when(j >= 1)
        def _():
            stage_b(j - 1)
        even = j % 2 == 0

        @pl.when(jnp.logical_and(even, j >= 2))
        def _():
            stage_c(j // 2 - 1)

        @pl.when(jnp.logical_and(jnp.logical_not(even), j >= 3))
        def _():
            stage_d((j - 3) // 2)

        @pl.when(jnp.logical_and(even, j >= 4))
        def _():
            stage_e(j // 2 - 2)
        return 0
    lax.fori_loop(0, NCH + 1, step, 0)

    def fin_cols(i, own):
        return (hi, far_cols[0], lo, own_cols[0])[2 * own + i]

    def t_yo(i, rows):
        return rc(YO + i, (xs, gs)[i].at[mine, fin_cols(i, False)], (y_out, dx_out)[i].at[rows, :], dev_y)

    def l_yo(i):
        return pltpu.make_async_copy((xs, gs)[i].at[mine, fin_cols(i, True)], (y_out, dx_out)[i].at[tok_rows, :],
                                     loc.at[8 + i])

    def finish(i):
        t_cp(i).wait_recv()
        acc, part, dst = (yacc, dxacc)[i], (yl, dl)[i], (xs, gs)[i]

        def fetch(q, slot):
            return pltpu.make_async_copy(part.at[pl.ds(pl.multiple_of(q * 128, 128), 128), :], stage.at[slot],
                                         isem.at[slot])
        fetch(0, 0).start()

        def piece(q, _):
            slot = q % 2

            @pl.when(q < 7)
            def _():
                fetch(q + 1, 1 - slot).start()
            fetch(q, slot).wait()
            rows = pl.ds(pl.multiple_of(q * 128, 128), 128)
            dst[rows, :] = (acc[rows, :] + stage[slot]).astype(BF16)
            return 0
        lax.fori_loop(0, 8, piece, 0)
        t_yo(i, tok_rows).start()
        l_yo(i).start()

    for i in (0, 1):
        t_tf(i).wait_send()
    finish(0)
    stage_d(3)
    finish(1)
    stage_e(3)

    def drain8(j, _):
        t_z2(j).wait_send()
        t_x1(j).wait_send()
        return 0
    lax.fori_loop(0, NCH, drain8, 0)

    def drain4(s, _):
        for t in (t_x2, t_y1, t_y2, t_z1, t_zo, t_c1):
            t(s).wait_send()
        t_zo_in(s).wait_recv()
        t_c1(s).wait_recv()
        l_o2(s).wait()
        l_o1(s).wait()
        return 0
    lax.fori_loop(0, NCH // 2, drain4, 0)

    def drain_w(s, _):
        for core in (0, 1):
            t_wy1(s, core, c).wait_send()
            t_wx1(s, core, c).wait_send()
        for t in (t_wp, t_wf1, t_wy2, t_wx2, t_wf2):
            t(s).wait_send()
        return 0
    lax.fori_loop(0, NCH // 2, drain_w, 0)
    for i in (0, 1):
        for t in (t_ty, t_tp, t_cp):
            t(i).wait_send()
        t_yo(i, tok_rows).wait_send()
        t_yo(i, oth_rows).wait_recv()
        l_yo(i).wait()


def fused(tok, grad, up, down):
    any_spec = pl.BlockSpec(memory_space=pl.ANY)
    vm = pltpu.VMEM
    shape = jax.ShapeDtypeStruct
    return pl.pallas_call(
        kernel,
        name="mlp_block",
        out_shape=(shape((TOK, HALF), BF16), shape((TOK, HALF), BF16), shape((2048, 256), F32), shape((1024, HALF), F32),
                   shape((TOK // 2, HID), F32), shape((TOK // 2, HID), F32),
                   shape((2, HID, HID), BF16), shape((2, HID, HID), BF16)),
        in_specs=[any_spec] * 4,
        out_specs=[any_spec] * 8,
        scratch_shapes=[
            vm((TOK, HID), BF16), vm((TOK, HID), BF16), vm((TOK, HID), F32), vm((TOK, HID), F32),
            vm((NCH, FC, HID), F32), vm((NCH, FC, HID), F32),
            vm((NCH, 128, HID), F32), vm((NCH, FC, HALF), F32),
            vm((4, 128, HID), F32), vm((4, 128, HALF), F32), vm((4, FC, HALF), F32), vm((4, FC, HALF), F32),
            vm((2, HID, FC), BF16), vm((2, FC, HID), BF16), vm((2, 128, HID), F32),
            pltpu.SemaphoreType.DMA((NSEM,)), pltpu.SemaphoreType.DMA((NSEM,)), pltpu.SemaphoreType.DMA((10,)),
            pltpu.SemaphoreType.DMA((2, 5)), pltpu.SemaphoreType.DMA((2,)),
        ],
        compiler_params=pltpu.CompilerParams(collective_id=0, has_side_effects=True, vmem_limit_bytes=67_043_328),
    )(tok, grad, up, down)


def solution(mesh):
    act_spec = P(("depth", "row"), "col")
    wgt_spec = P("row", "col")

    def block(tok, up, down, grad):
        out = fused(tok, grad, up, down)
        return out[0], out[1], out[2].T, out[3]

    return jax.shard_map(block, mesh=mesh, in_specs=(act_spec, wgt_spec, wgt_spec, act_spec),
                         out_specs=(act_spec, act_spec, wgt_spec, wgt_spec), check_vma=False)
```

```python
import math
import jax
import jax.numpy as jnp
from jax import lax
from jax.experimental import pallas as pl
from jax.experimental.pallas import tpu as pltpu
from jax.sharding import PartitionSpec as P

INV_ROOT_TWO = 1.0 / math.sqrt(2.0)
INV_ROOT_TAU = 1.0 / math.sqrt(2.0 * math.pi)
MESH = pl.DeviceIdType.MESH
BF16, F32 = jnp.bfloat16, jnp.float32

TOK, HID, FC, NCH = 2048, 1024, 256, 8
HALF, TILE, ROWS = 512, 512, 128
NT = TOK // TILE
FIRST = ("wy0", "t0", "wy1", "t1", "wy2", "wy3", "wxo0", "wxo1", "wxo2", "wxo3",)
ORDERS = {1: ("ZCB", "CZB", "CBZ", "CZB"),
          2: ("CZB", "CBZ", "CBZ", "ZBC")}
PLAN = {
    0: ("fw0", "fzx0", "fzx1", "fzx2", "fzx3", "ft0", "fz0", "fw1", "fz1", "lw0", "lw1",),
    2: ("ft1",),
    4: ("fw2", "lw2", "s1000", "s2000",),
    6: ("fw3",),
    8: ("fz2", "lw3", "s1001", "s2001",),
    10: ("fz3", "b1000",),
    11: ("b2000",),
    12: ("s1100", "s2100",),
    15: ("lw4", "b2001", "s201",),
    16: ("lw5", "s1101", "s2101",),
    18: ("b1100",),
    19: ("b1001", "s101",),
    20: ("s1200", "s2200", "b2100",),
    22: ("b1101", "s111",),
    23: ("lw6",),
    24: ("lw7", "s1201", "s2201", "b2101", "s211",),
    26: ("b101", "s102",),
    28: ("s1300", "s2300", "b201", "b2200", "s202",),
    31: ("b1200",),
    32: ("cp", "s1301", "s2301", "b111", "s112", "b2201", "s221", "b102", "b1201", "s121", "b2300", "fin0",
        "b112", "b211", "s212", "fin1", "b2301", "b121", "s231", "s122", "b1300", "b202", "b212", "b1301",
        "s131", "b122", "b221", "s222", "b231", "s232", "b131", "s132", "b232", "b132", "b222",),
}

def dot(a, b, ca, cb):
    return lax.dot_general(a, b, (((ca,), (cb,)), ((), ())), preferred_element_type=F32)


def hop_shapes(order):
    nb, rows, cols, shapes = 2, FC, HID, []
    for h, kind in enumerate(order):
        if kind == "B":
            nb = 1
        elif kind == "C":
            cols = HALF
        elif h < 2:
            rows = ROWS
        shapes.append((nb, rows, cols))
    return shapes


def kernel(x_in, g_in, up_in, down_in, y_out, dx_out, d1_out, d2_out, yl, dl, w1b, w2b,
           xs, gs, yacc, dxacc, d1, d2, w1s, w2s, send, recv, loc, wsem, isem, *land):
    z, y, r = lax.axis_index("depth"), lax.axis_index("col"), lax.axis_index("row")
    x, c = r // 2, r % 2
    r_x = (1 - x) * 2 + c
    r_c = r + 1 - 2 * c
    dev_c, dev_x, dev_xc = (z, y, r_c), (z, y, r_x), (z, y, (1 - x) * 2 + 1 - c)
    dev_y, dev_yc, dev_z, dev_zc = (z, 1 - y, r), (z, 1 - y, r_c), (1 - z, y, r), (1 - z, y, r_c)
    everything, lo, hi = slice(None), pl.ds(0, HALF), pl.ds(HALF, HALF)
    zrow = pl.ds(pl.multiple_of(z * ROWS, ROWS), ROWS)
    zoth = pl.ds(pl.multiple_of((1 - z) * ROWS, ROWS), ROWS)
    slots = {}

    def slot_of(name):
        return slots.setdefault(name, len(slots))

    def rc(name, src, dst, dev, arrives=None):
        return pltpu.make_async_remote_copy(
            src_ref=src, dst_ref=dst, send_sem=send.at[slot_of(name)],
            recv_sem=recv.at[slot_of(name if arrives is None else arrives)], device_id=dev, device_id_type=MESH)

    def go(*copies):
        for cp in copies:
            cp.start()

    def got(*copies):
        for cp in copies:
            cp.wait_recv()

    barrier = pltpu.get_barrier_semaphore()
    for dev in (dev_c, dev_x, dev_xc, dev_y, dev_yc, dev_z, dev_zc):
        pl.semaphore_signal(barrier, inc=1, device_id=dev, device_id_type=MESH)
    pl.semaphore_wait(barrier, 7)

    def chunk(q):
        return pl.ds(pl.multiple_of(q * FC, FC), FC)

    def up_cols(core, s):
        return pl.ds(pl.multiple_of(core * HID + s * FC, FC), FC)

    def part(xh, core, zi):
        return pl.ds(pl.multiple_of(xh * HALF + core * FC + zi * ROWS, ROWS), ROWS)

    def down_rows(s):
        return pl.ds(pl.multiple_of(s * FC + z * ROWS, ROWS), ROWS)

    def by_core(name, s, core, src, dst, dev):
        base = slot_of(f"{name}{s}0")
        slot_of(f"{name}{s}1")
        return pltpu.make_async_remote_copy(src_ref=src, dst_ref=dst, send_sem=send.at[base + core],
                                            recv_sem=recv.at[base + c], device_id=dev, device_id_type=MESH)

    def by_core_in(name, s, core, like):
        base = slot_of(f"{name}{s}0")
        slot_of(f"{name}{s}1")
        return pltpu.make_async_remote_copy(src_ref=like, dst_ref=like, send_sem=send.at[base + core],
                                            recv_sem=recv.at[base + core], device_id=dev_c, device_id_type=MESH)

    def wy(s):
        two = [by_core("wy", s, q, up_in.at[zrow, up_cols(q, s)], w1b.at[y, part(0, c, z), chunk(s)], (z, 1 - y, x * 2 + q))
               for q in (0, 1)]
        return two + [wy_down(s)]

    def wy_down(s):
        return rc(f"wY{s}", down_in.at[down_rows(s), :], w2b.at[x, down_rows(s), hi], dev_y)

    def wy_in(s):
        return [by_core_in("wy", s, q, w1b.at[1 - y, part(0, q, z), chunk(s)]) for q in (0, 1)] + [wy_down(s)]

    def wx(s):
        two = [by_core("wx", s, q, up_in.at[zrow, up_cols(q, s)], w1b.at[y, part(1, c, z), chunk(s)],
                       (z, y, (1 - x) * 2 + q)) for q in (0, 1)]
        return two + [wx_down(s)]

    def wx_down(s):
        return rc(f"wX{s}", down_in.at[down_rows(s), :], w2b.at[x, down_rows(s), lo], dev_x)

    def wx_in(s):
        return [by_core_in("wx", s, q, w1b.at[y, part(1, q, z), chunk(s)]) for q in (0, 1)] + [wx_down(s)]

    def wp(s):
        return [rc(f"wp{s}", up_in.at[:, up_cols(1 - c, s)], w1b.at[y, chunk(c), chunk(s)], dev_c)]

    def wf(s):
        two = [rc(f"wf{s}{q}", w1b.at[1 - y, part(0, q, z), chunk(s)], w1b.at[1 - y, part(1, q, z), chunk(s)], dev_x)
               for q in (0, 1)]
        both = w2b.at[x, down_rows(s), hi]
        return two + [rc(f"wF{s}", both, both, dev_x)]

    def same_z(name, ref):
        return rc(name, ref, ref, dev_z)

    def wzx(s):
        return [same_z(f"wzx{s}{q}", w1b.at[y, part(1, q, z), chunk(s)]) for q in (0, 1)] + [
            same_z(f"wzX{s}", w2b.at[1 - x, down_rows(s), lo])]

    def wz(s):
        return [same_z(f"wz{s}{h}{q}", w1b.at[1 - y, part(h, q, z), chunk(s)]) for h in (0, 1) for q in (0, 1)] + [
            same_z(f"wZ{s}{i}", w2b.at[(x, 1 - x)[i], down_rows(s), hi]) for i in (0, 1)]

    def load_w(j, slot, start):
        s, b = j // 2, j % 2

        def cp(src, dst, k):
            copy = pltpu.make_async_copy(src, dst, wsem.at[slot, k])
            copy.start() if start else copy.wait()
        v1, v2 = w1s.at[slot], w2s.at[slot]
        if start:
            @pl.when(b == y)
            def _():
                cp(up_in.at[:, up_cols(c, s)], v1.at[chunk(c), :], 0)

            @pl.when(b != y)
            def _():
                cp(w1b.at[b, chunk(c), chunk(s)], v1.at[chunk(c), :], 0)

            @pl.when(b == x)
            def _():
                cp(down_in.at[chunk(s), :], v2.at[:, lo], 3)

            @pl.when(b != x)
            def _():
                cp(w2b.at[b, chunk(s), lo], v2.at[:, lo], 3)
        else:
            cp(up_in.at[:, up_cols(c, s)], v1.at[chunk(c), :], 0)
            cp(down_in.at[chunk(s), :], v2.at[:, lo], 3)
        cp(w1b.at[b, chunk(1 - c), chunk(s)], v1.at[chunk(1 - c), :], 1)
        cp(w1b.at[b, hi, chunk(s)], v1.at[hi, :], 2)
        cp(w2b.at[b, chunk(s), hi], v2.at[:, hi], 4)

    own_cols = (pl.ds(pl.multiple_of(jnp.where(x == y, 0, HALF), HALF), HALF), lo)
    far_cols = (pl.ds(pl.multiple_of(jnp.where(x == y, HALF, 0), HALF), HALF), hi)
    ins, tok = (x_in, g_in), (xs, gs)

    def tok_at(base, i):
        return pl.ds(pl.multiple_of(base * (TOK // 2) + i * TILE, TILE), TILE)

    def ty(i):
        return [rc(f"ty{i}{k}", ins[k].at[tok_at(1 - y, i), :], tok[k].at[tok_at(0, i), (own_cols[0], hi)[k]], dev_y)
                for k in (0, 1)]

    def tp(i):
        return [rc(f"tp{i}{k}", ins[k].at[tok_at(y, i), :], tok[k].at[tok_at(1, i), own_cols[k]], dev_c) for k in (0, 1)]

    def tf(i):
        return [rc(f"tf{i}{k}", tok[k].at[tok_at(0, i), far_cols[k]], tok[k].at[tok_at(1, i), far_cols[k]], dev_c)
                for k in (0, 1)]

    def tl(i):
        return [pltpu.make_async_copy(ins[k].at[tok_at(y, i), :], tok[k].at[tok_at(0, i), own_cols[k]],
                                      isem.at[2 * i + k]) for k in (0, 1)]

    parts = {1: d1, 2: d2}
    buf = {(m, s, h): land[(m - 1) * 12 + s * 3 + h] for m in (1, 2) for s in range(4) for h in range(3)}
    keep_block = {1: y, 2: x}
    dev_of = {(1, "C"): dev_x, (1, "B"): dev_y, (1, "Z"): dev_z, (2, "C"): dev_y, (2, "B"): dev_x, (2, "Z"): dev_z}

    def live(m, s, h):
        blocks, rows, cols = [2 * s, 2 * s + 1], everything, everything
        for kind in ORDERS[m][s][:h]:
            if kind == "B":
                blocks = [2 * s + keep_block[m]]
            elif kind == "C":
                cols = lo
            else:
                rows = zrow
        return blocks, rows, cols

    def hop(m, s, h, only=None):
        kind = ORDERS[m][s][h]
        blocks, rows, cols = live(m, s, h)
        d, b, dev = parts[m], buf[m, s, h], dev_of[m, kind]
        if kind == "B":
            ends = [(d.at[2 * s + 1 - keep_block[m], rows, cols], (2 * s + keep_block[m], rows, cols))]
        elif kind == "C":
            ends = [(d.at[q, rows, hi], (q, rows, lo)) for q in blocks]
        elif h < 2:
            ends = [(d.at[q, zoth, cols], (q, zrow, cols)) for q in blocks]
        else:
            ends = [(d.at[q, rows, cols], (q, rows, cols)) for q in blocks]
        return [(rc(f"h{m}{s}{h}{i}", src, b.at[i], dev), b.at[i], into)
                for i, (src, into) in enumerate(ends) if only is None or i == only]

    def add_hop(m, s, h, only=None):
        for cp, landed, (q, rows, cols) in hop(m, s, h, only):
            got(cp)
            if h < 2:
                parts[m][q, rows, cols] += landed[...]
            else:
                landed[...] += parts[m][q, rows, cols]
        if h == 2:
            go(*gives(m, s))
            for cp in stores(m, s):
                cp.start()

    def fin_rows(m, s, other=False):
        split = ORDERS[m][s][2] != "Z"
        base = s * FC + (c * HID if m == 1 else 0)
        if split:
            base = base + ((1 - z) if other else z) * ROWS
        return pl.ds(pl.multiple_of(base, ROWS), ROWS if split else FC)

    def cols_c(q):
        return pl.ds(pl.multiple_of(q * 256, 256), 256)

    def gives(m, s):
        b, split = buf[m, s, 2], ORDERS[m][s][2] != "Z"
        rows = fin_rows(m, s)
        if m == 2:
            return [rc(f"a2{s}", b.at[0], d2_out.at[rows, :], dev_z)] if split else []
        out = [rc(f"c1{s}", b.at[0, :, cols_c(1 - c)], d1_out.at[rows, :], dev_c)]
        if split:
            out += [rc(f"a1{s}", b.at[0, :, cols_c(c)], d1_out.at[rows, :], dev_z),
                    rc(f"k1{s}", b.at[0, :, cols_c(1 - c)], d1_out.at[rows, :], dev_zc)]
        return out

    def stores(m, s):
        b = buf[m, s, 2]
        if m == 2:
            return [pltpu.make_async_copy(b.at[0], d2_out.at[fin_rows(m, s), :], loc.at[4 + s])]
        return [pltpu.make_async_copy(b.at[0, :, cols_c(c)], d1_out.at[fin_rows(m, s), :], loc.at[s])]

    mine, theirs = pl.ds(0, TOK // 2), pl.ds(TOK // 2, TOK // 2)

    def t_cp(i):
        return rc(f"cp{i}", (yacc, dxacc)[i].at[theirs, :], (yl, dl)[i], dev_c)

    def out_rows(q):
        return pl.ds(pl.multiple_of(q * (TOK // 2), TOK // 2), TOK // 2)

    def t_yo(i):
        cols = (hi, far_cols[0])[i]
        return rc(f"yo{i}", (xs, gs)[i].at[mine, cols], (y_out, dx_out)[i].at[out_rows(y), :], dev_y)

    def l_yo(i):
        cols = (lo, own_cols[0])[i]
        return pltpu.make_async_copy((xs, gs)[i].at[mine, cols], (y_out, dx_out)[i].at[out_rows(y), :], loc.at[8 + i])

    stage = None
    for m, s in ((m, s) for s in range(4) for m in (1, 2)):
        b = buf[m, s, 0]
        if stage is None and b.shape != (2, FC, HALF):
            stage = [b.at[0], b.at[1]] if b.shape[0] == 2 else [b.at[0, pl.ds(0, ROWS)], b.at[0, pl.ds(ROWS, ROWS)]]

    def finish(i):
        got(t_cp(i))
        acc, piece, dst = (yacc, dxacc)[i], (yl, dl)[i], (xs, gs)[i]

        def fetch(q, k):
            rows = pl.ds(pl.multiple_of(q * ROWS, ROWS), ROWS)
            return pltpu.make_async_copy(piece.at[rows, :], stage[k], isem.at[k])
        fetch(0, 0).start()

        def two(p, _):
            for k in (0, 1):
                q = 2 * p + k

                @pl.when(q + 1 < TOK // 2 // ROWS)
                def _():
                    fetch(q + 1, 1 - k).start()
                fetch(q, k).wait()
                rows = pl.ds(pl.multiple_of(q * ROWS, ROWS), ROWS)
                dst[rows, :] = (acc[rows, :] + stage[k][...]).astype(BF16)
            return 0
        lax.fori_loop(0, TOK // 2 // ROWS // 2, two, 0)
        go(t_yo(i))
        l_yo(i).start()

    def event(name):
        kind, a = name.rstrip("0123456789a"), name
        n = int(name[-1]) if name[-1].isdigit() else None
        if kind == "wy":
            go(*wy(n))
        elif kind == "wxo":
            go(*wx(n), *wp(n))
        elif kind == "t":
            go(*ty(n), *tp(n))
            for cp in tl(n):
                cp.start()
        elif kind == "fw":
            got(*wy_in(n))
            go(*wf(n))
        elif kind == "fzx":
            got(*wx_in(n))
            go(*wzx(n))
        elif kind == "fz":
            got(*wf(n))
            go(*wz(n))
        elif kind == "lw":
            if n % 2 == 0:
                got(*wzx(n // 2), *wz(n // 2), *wp(n // 2))
            load_w(n, n % 2, True)
        elif kind == "ft":
            got(*ty(n))
            go(*tf(n))
            for cp in tl(n):
                cp.wait()
        elif kind == "fr":
            got(*tp(n), *tf(n))
        elif kind in ("s", "b"):
            m, s, h = int(a[1]), int(a[2]), int(a[3])
            only = int(a[4]) if len(a) > 4 and a[4] != "a" else None
            if kind == "s":
                go(*[q[0] for q in hop(m, s, h, only)])
            else:
                add_hop(m, s, h, only)
        elif kind == "cp":
            go(t_cp(0), t_cp(1))
            for i in (0, 1):
                for cp in tf(i):
                    cp.wait_send()
        elif kind == "fin":
            finish(n)

    for name in FIRST:
        event(name)

    def zero(i, _):
        rows = pl.ds(pl.multiple_of(i * 64, 64), 64)
        yacc[rows, :] = jnp.zeros((64, HID), F32)
        dxacc[rows, :] = jnp.zeros((64, HID), F32)
        return 0
    lax.fori_loop(0, TOK // 64, zero, 0)

    plan = {n: list(v) for n, v in PLAN.items()}
    plan.setdefault(1, []).append("fr0")
    plan.setdefault(3, []).append("fr1")
    for name in plan[0]:
        event(name)

    def tile(n, _):
        for at in sorted(plan):
            if 0 < at < NCH * NT:
                @pl.when(n == at)
                def _():
                    for name in plan[at]:
                        event(name)
        j, q = n // NT, n % NT
        slot = j % 2

        @pl.when(q == 0)
        def _():
            load_w(j, slot, False)
        w1, w2 = w1s.at[slot], w2s.at[slot]
        t = (q % 2) * 2 + q // 2
        rows = pl.ds(pl.multiple_of(t * TILE, TILE), TILE)
        xt, gt = xs[rows, :], gs[rows, :]
        u = dot(xt, w1[...], 1, 0)
        da = dot(gt, w2[...], 1, 1)
        cdf = 0.5 * (1.0 + lax.erf(u * INV_ROOT_TWO))
        act = (u * cdf).astype(BF16)
        du = (da * (cdf + u * jnp.exp(-0.5 * u * u) * INV_ROOT_TAU)).astype(BF16)
        yacc[rows, :] += dot(act, w2[...], 1, 0)
        dxacc[rows, :] += dot(du, w1[...], 1, 1)
        p2, p1 = dot(act, gt, 0, 0), dot(du, xt, 0, 0)

        @pl.when(q == 0)
        def _():
            d2[j] = p2
            d1[j] = p1

        @pl.when(q > 0)
        def _():
            d2[j] += p2
            d1[j] += p1
        return 0
    lax.fori_loop(0, NCH * NT, tile, 0)
    for name in plan[NCH * NT]:
        event(name)

    for s in range(4):
        for cp in wy(s) + wx(s) + wp(s) + wf(s) + wzx(s) + wz(s):
            cp.wait_send()
        for m in (1, 2):
            for h in range(3):
                for cp, _, _ in hop(m, s, h):
                    cp.wait_send()
            for cp in gives(m, s):
                cp.wait_send()
                cp.wait_recv()
            for cp in stores(m, s):
                cp.wait()
    for i in (0, 1):
        for cp in ty(i) + tp(i) + [t_cp(i), t_yo(i)]:
            cp.wait_send()
        got(t_yo(i))
        l_yo(i).wait()


def fused(tok, grad, up, down):
    any_spec = pl.BlockSpec(memory_space=pl.ANY)
    vm, shape = pltpu.VMEM, jax.ShapeDtypeStruct
    land = [vm(dims, F32) for m in (1, 2) for s in range(4) for dims in hop_shapes(ORDERS[m][s])]
    dma = pltpu.SemaphoreType.DMA
    return pl.pallas_call(
        kernel,
        name="mlp_block",
        out_shape=(shape((TOK, HALF), BF16), shape((TOK, HALF), BF16), shape((2048, 256), F32), shape((1024, HALF), F32),
                   shape((TOK // 2, HID), F32), shape((TOK // 2, HID), F32),
                   shape((2, HID, HID), BF16), shape((2, HID, HID), BF16)),
        in_specs=[any_spec] * 4,
        out_specs=[any_spec] * 8,
        scratch_shapes=[
            vm((TOK, HID), BF16), vm((TOK, HID), BF16), vm((TOK, HID), F32), vm((TOK, HID), F32),
            vm((NCH, FC, HID), F32), vm((NCH, FC, HID), F32), vm((2, HID, FC), BF16), vm((2, FC, HID), BF16),
            dma((160,)), dma((160,)), dma((10,)), dma((2, 5)), dma((4,)), *land,
        ],
        compiler_params=pltpu.CompilerParams(collective_id=0, has_side_effects=True, vmem_limit_bytes=67_043_328),
    )(tok, grad, up, down)


def solution(mesh):
    act_spec = P(("depth", "row"), "col")
    wgt_spec = P("row", "col")

    def block(tok, up, down, grad):
        out = fused(tok, grad, up, down)
        return out[0], out[1], out[2].T, out[3]

    return jax.shard_map(block, mesh=mesh, in_specs=(act_spec, wgt_spec, wgt_spec, act_spec),
                         out_specs=(act_spec, act_spec, wgt_spec, wgt_spec), check_vma=False)
```

```python
import math
import jax
import jax.numpy as jnp
from jax import lax
from jax.experimental import pallas as pl
from jax.experimental.pallas import tpu as pltpu
from jax.sharding import PartitionSpec as P

INV_ROOT_TWO = 1.0 / math.sqrt(2.0)
INV_ROOT_TAU = 1.0 / math.sqrt(2.0 * math.pi)
MESH = pl.DeviceIdType.MESH
BF16, F32 = jnp.bfloat16, jnp.float32

TOK, HID, FC, NCH = 2048, 1024, 256, 8
HALF, TILE, ROWS = 512, 512, 128
NT = TOK // TILE
ROUTES = "BAAB"
ORDERS = {1: ("CBZ", "ZBC", "ZCB", "BCZ"),
          2: ("CBZ", "CBZ", "BZC", "BZC")}
PLAN = {
    0: ("gwxo0", "gwy1", "gwxo1", "gwy0", "gwxo2", "gt0", "fzx0", "fw1", "gwzx0", "gwxf1", "fzx1", "fw0",
        "gwz0", "gwzx1", "gwxo3", "fzx2", "gwzx2", "fz0", "gwxf0", "fz1", "gwz1", "gt1", "fzx3", "ft0",
        "gwzx3", "lw0", "lw1",),
    2: ("gwy2", "gwy3", "ft1",),
    4: ("fw2", "lw2", "gwxf2", "gh2000",),
    5: ("gh1000",),
    6: ("fw3", "gwz3",),
    8: ("fz2", "lw3", "gh2001", "gwz2",),
    9: ("gh1001",),
    10: ("fz3",),
    11: ("b2000",),
    12: ("b1000", "gh2100", "gh1100",),
    14: ("lw4", "gwxf3",),
    15: ("b2001",),
    16: ("lw5", "gh1101",),
    17: ("b1001", "gh101",),
    18: ("gh201",),
    19: ("b1100",),
    20: ("b2100", "gh1200",),
    21: ("lw6", "gh2101",),
    23: ("b1101",),
    24: ("lw7", "b101", "gh2200",),
    25: ("gh102",),
    26: ("b201", "gh111",),
    28: ("b1200",),
    29: ("b2101", "gh202",),
    32: ("cp", "gh2300", "gh1300", "b102", "b111", "gh1201", "b2200", "fin00", "b202", "fin01", "gh221",
        "gyo01", "fin10", "fin11", "b1201", "gh112", "b1300", "gh211", "gyo11", "b2300", "gh231", "b221",
        "b112", "ga11", "gh121", "gh222", "b231", "gh232", "b211", "gh212", "gh131", "gyo10", "b222",
        "ga22", "b121", "b232", "ga23", "b212", "gh122", "gyo00", "b131", "gh132", "b122", "ga12", "b132",),
}

def dot(a, b, ca, cb):
    return lax.dot_general(a, b, (((ca,), (cb,)), ((), ())), preferred_element_type=F32)


def hop_shapes(order):
    nb, rows, cols, shapes = 2, FC, HID, []
    for h, kind in enumerate(order):
        if kind == "B":
            nb = 1
        elif kind == "C":
            cols = HALF
        elif h < 2:
            rows = ROWS
        shapes.append((nb, rows, cols))
    return shapes


def kernel(x_in, g_in, up_in, down_in, y_out, dx_out, d1_out, d2_out, yl, dl, w1b, w2b,
           xs, gs, yacc, dxacc, d1, d2, w1s, w2s, send, recv, loc, wsem, isem, *land):
    z, y, r = lax.axis_index("depth"), lax.axis_index("col"), lax.axis_index("row")
    x, c = r // 2, r % 2
    r_x = (1 - x) * 2 + c
    r_c = r + 1 - 2 * c
    dev_c, dev_x, dev_xc = (z, y, r_c), (z, y, r_x), (z, y, (1 - x) * 2 + 1 - c)
    dev_y, dev_yc, dev_z, dev_zc = (z, 1 - y, r), (z, 1 - y, r_c), (1 - z, y, r), (1 - z, y, r_c)
    everything, lo, hi = slice(None), pl.ds(0, HALF), pl.ds(HALF, HALF)
    zrow = pl.ds(pl.multiple_of(z * ROWS, ROWS), ROWS)
    zoth = pl.ds(pl.multiple_of((1 - z) * ROWS, ROWS), ROWS)
    slots = {}

    def slot_of(name):
        return slots.setdefault(name, len(slots))

    def rc(name, src, dst, dev, arrives=None):
        return pltpu.make_async_remote_copy(
            src_ref=src, dst_ref=dst, send_sem=send.at[slot_of(name)],
            recv_sem=recv.at[slot_of(name if arrives is None else arrives)], device_id=dev, device_id_type=MESH)

    def go(*copies):
        for cp in copies:
            cp.start()

    def got(*copies):
        for cp in copies:
            cp.wait_recv()

    barrier = pltpu.get_barrier_semaphore()
    for dev in (dev_c, dev_x, dev_xc, dev_y, dev_yc, dev_z, dev_zc):
        pl.semaphore_signal(barrier, inc=1, device_id=dev, device_id_type=MESH)
    pl.semaphore_wait(barrier, 7)

    def chunk(q):
        return pl.ds(pl.multiple_of(q * FC, FC), FC)

    def up_cols(core, s):
        return pl.ds(pl.multiple_of(core * HID + s * FC, FC), FC)

    def part(xh, core, zi):
        return pl.ds(pl.multiple_of(xh * HALF + core * FC + zi * ROWS, ROWS), ROWS)

    def down_rows(s):
        return pl.ds(pl.multiple_of(s * FC + z * ROWS, ROWS), ROWS)

    def by_core(name, s, core, src, dst, dev):
        base = slot_of(f"{name}{s}0")
        slot_of(f"{name}{s}1")
        return pltpu.make_async_remote_copy(src_ref=src, dst_ref=dst, send_sem=send.at[base + core],
                                            recv_sem=recv.at[base + c], device_id=dev, device_id_type=MESH)

    def by_core_in(name, s, core, like):
        base = slot_of(f"{name}{s}0")
        slot_of(f"{name}{s}1")
        return pltpu.make_async_remote_copy(src_ref=like, dst_ref=like, send_sem=send.at[base + core],
                                            recv_sem=recv.at[base + core], device_id=dev_c, device_id_type=MESH)

    def wy(s):
        two = [by_core("wy", s, q, up_in.at[zrow, up_cols(q, s)], w1b.at[y, part(0, c, z), chunk(s)], (z, 1 - y, x * 2 + q))
               for q in (0, 1)]
        return two + [wy_down(s)]

    def wy_down(s):
        return rc(f"wY{s}", down_in.at[down_rows(s), :], w2b.at[x, down_rows(s), hi], dev_y)

    def wy_in(s):
        return [by_core_in("wy", s, q, w1b.at[1 - y, part(0, q, z), chunk(s)]) for q in (0, 1)] + [wy_down(s)]

    def wx(s):
        two = [by_core("wx", s, q, up_in.at[zrow, up_cols(q, s)], w1b.at[y, part(1, c, z), chunk(s)],
                       (z, y, (1 - x) * 2 + q)) for q in (0, 1)]
        return two + [wx_down(s)]

    def wx_down(s):
        return rc(f"wX{s}", down_in.at[down_rows(s), :], w2b.at[x, down_rows(s), lo], dev_x)

    def wx_in(s):
        return [by_core_in("wx", s, q, w1b.at[y, part(1, q, z), chunk(s)]) for q in (0, 1)] + [wx_down(s)]

    def wp(s):
        return [rc(f"wp{s}", up_in.at[:, up_cols(1 - c, s)], w1b.at[y, chunk(c), chunk(s)], dev_c)]

    def wxf(s):
        if ROUTES[s] == "B":
            both = w2b.at[x, chunk(s), hi]
            return [rc(f"wf{s}0", w1b.at[1 - y, lo, chunk(s)], w1b.at[1 - y, hi, chunk(s)], dev_x),
                    rc(f"wF{s}", both, both, dev_x)]
        two = [rc(f"wf{s}{q}", w1b.at[1 - y, part(0, q, z), chunk(s)], w1b.at[1 - y, part(1, q, z), chunk(s)], dev_x)
               for q in (0, 1)]
        both = w2b.at[x, down_rows(s), hi]
        return two + [rc(f"wF{s}", both, both, dev_x)]

    def same_z(name, ref):
        return rc(name, ref, ref, dev_z)

    def wzx(s):
        return [same_z(f"wzx{s}{q}", w1b.at[y, part(1, q, z), chunk(s)]) for q in (0, 1)] + [
            same_z(f"wzX{s}", w2b.at[1 - x, down_rows(s), lo])]

    def wz(s):
        if ROUTES[s] == "B":
            return [same_z(f"wz{s}0{q}", w1b.at[1 - y, part(0, q, z), chunk(s)]) for q in (0, 1)] + [
                same_z(f"wZ{s}0", w2b.at[x, down_rows(s), hi])]
        return [same_z(f"wz{s}{h}{q}", w1b.at[1 - y, part(h, q, z), chunk(s)]) for h in (0, 1) for q in (0, 1)] + [
            same_z(f"wZ{s}{i}", w2b.at[(x, 1 - x)[i], down_rows(s), hi]) for i in (0, 1)]

    def load_w(j, slot, start):
        s, b = j // 2, j % 2

        def cp(src, dst, k):
            copy = pltpu.make_async_copy(src, dst, wsem.at[slot, k])
            copy.start() if start else copy.wait()
        v1, v2 = w1s.at[slot], w2s.at[slot]
        if start:
            @pl.when(b == y)
            def _():
                cp(up_in.at[:, up_cols(c, s)], v1.at[chunk(c), :], 0)

            @pl.when(b != y)
            def _():
                cp(w1b.at[b, chunk(c), chunk(s)], v1.at[chunk(c), :], 0)

            @pl.when(b == x)
            def _():
                cp(down_in.at[chunk(s), :], v2.at[:, lo], 3)

            @pl.when(b != x)
            def _():
                cp(w2b.at[b, chunk(s), lo], v2.at[:, lo], 3)
        else:
            cp(up_in.at[:, up_cols(c, s)], v1.at[chunk(c), :], 0)
            cp(down_in.at[chunk(s), :], v2.at[:, lo], 3)
        cp(w1b.at[b, chunk(1 - c), chunk(s)], v1.at[chunk(1 - c), :], 1)
        cp(w1b.at[b, hi, chunk(s)], v1.at[hi, :], 2)
        cp(w2b.at[b, chunk(s), hi], v2.at[:, hi], 4)

    own_cols = (pl.ds(pl.multiple_of(jnp.where(x == y, 0, HALF), HALF), HALF), lo)
    far_cols = (pl.ds(pl.multiple_of(jnp.where(x == y, HALF, 0), HALF), HALF), hi)
    ins, tok = (x_in, g_in), (xs, gs)

    def tok_at(base, i):
        return pl.ds(pl.multiple_of(base * (TOK // 2) + i * TILE, TILE), TILE)

    def ty(i):
        return [rc(f"ty{i}{k}", ins[k].at[tok_at(1 - y, i), :], tok[k].at[tok_at(0, i), (own_cols[0], hi)[k]], dev_y)
                for k in (0, 1)]

    def tp(i):
        return [rc(f"tp{i}{k}", ins[k].at[tok_at(y, i), :], tok[k].at[tok_at(1, i), own_cols[k]], dev_c) for k in (0, 1)]

    def tf(i):
        return [rc(f"tf{i}{k}", tok[k].at[tok_at(0, i), far_cols[k]], tok[k].at[tok_at(1, i), far_cols[k]], dev_c)
                for k in (0, 1)]

    def tl(i):
        return [pltpu.make_async_copy(ins[k].at[tok_at(y, i), :], tok[k].at[tok_at(0, i), own_cols[k]],
                                      isem.at[2 * i + k]) for k in (0, 1)]

    parts = {1: d1, 2: d2}
    buf = {(m, s, h): land[(m - 1) * 12 + s * 3 + h] for m in (1, 2) for s in range(4) for h in range(3)}
    keep_block = {1: y, 2: x}
    dev_of = {(1, "C"): dev_x, (1, "B"): dev_y, (1, "Z"): dev_z, (2, "C"): dev_y, (2, "B"): dev_x, (2, "Z"): dev_z}

    def live(m, s, h):
        blocks, rows, cols = [2 * s, 2 * s + 1], everything, everything
        for kind in ORDERS[m][s][:h]:
            if kind == "B":
                blocks = [2 * s + keep_block[m]]
            elif kind == "C":
                cols = lo
            else:
                rows = zrow
        return blocks, rows, cols

    def hop(m, s, h, only=None):
        kind = ORDERS[m][s][h]
        blocks, rows, cols = live(m, s, h)
        d, b, dev = parts[m], buf[m, s, h], dev_of[m, kind]
        if kind == "B":
            ends = [(d.at[2 * s + 1 - keep_block[m], rows, cols], (2 * s + keep_block[m], rows, cols))]
        elif kind == "C":
            ends = [(d.at[q, rows, hi], (q, rows, lo)) for q in blocks]
        elif h < 2:
            ends = [(d.at[q, zoth, cols], (q, zrow, cols)) for q in blocks]
        else:
            ends = [(d.at[q, rows, cols], (q, rows, cols)) for q in blocks]
        return [(rc(f"h{m}{s}{h}{i}", src, b.at[i], dev), b.at[i], into)
                for i, (src, into) in enumerate(ends) if only is None or i == only]

    def add_hop(m, s, h, only=None):
        for cp, landed, (q, rows, cols) in hop(m, s, h, only):
            got(cp)
            if h < 2:
                parts[m][q, rows, cols] += landed[...]
            else:
                landed[...] += parts[m][q, rows, cols]
        if h == 2:
            go(*gives(m, s, False))
            for cp in stores(m, s):
                cp.start()

    def fin_rows(m, s, other=False):
        split = ORDERS[m][s][2] != "Z"
        base = s * FC + (c * HID if m == 1 else 0)
        if split:
            base = base + ((1 - z) if other else z) * ROWS
        return pl.ds(pl.multiple_of(base, ROWS), ROWS if split else FC)

    def cols_c(q):
        return pl.ds(pl.multiple_of(q * 256, 256), 256)

    def gives(m, s, far):
        b, split = buf[m, s, 2], ORDERS[m][s][2] != "Z"
        rows = fin_rows(m, s)
        if far and not split or m == 2 and not far:
            return []
        if m == 2:
            return [rc(f"a2{s}", b.at[0], d2_out.at[rows, :], dev_z)]
        if not far:
            return [rc(f"c1{s}", b.at[0, :, cols_c(1 - c)], d1_out.at[rows, :], dev_c)]
        return [rc(f"a1{s}", b.at[0, :, cols_c(c)], d1_out.at[rows, :], dev_z),
                rc(f"k1{s}", b.at[0, :, cols_c(1 - c)], d1_out.at[rows, :], dev_zc)]

    def stores(m, s):
        b = buf[m, s, 2]
        if m == 2:
            return [pltpu.make_async_copy(b.at[0], d2_out.at[fin_rows(m, s), :], loc.at[4 + s])]
        return [pltpu.make_async_copy(b.at[0, :, cols_c(c)], d1_out.at[fin_rows(m, s), :], loc.at[s])]

    mine, theirs = pl.ds(0, TOK // 2), pl.ds(TOK // 2, TOK // 2)

    def t_cp(i):
        return rc(f"cp{i}", (yacc, dxacc)[i].at[theirs, :], (yl, dl)[i], dev_c)

    def out_rows(k):
        return pl.ds(pl.multiple_of(y * (TOK // 2) + k * HALF, HALF), HALF)

    def t_yo(i, k):
        return rc(f"yo{i}{k}", (xs, gs)[i].at[pl.ds(k * HALF, HALF), (hi, far_cols[0])[i]],
                  (y_out, dx_out)[i].at[out_rows(k), :], dev_y)

    def l_yo(i, k):
        return pltpu.make_async_copy((xs, gs)[i].at[pl.ds(k * HALF, HALF), (lo, own_cols[0])[i]],
                                     (y_out, dx_out)[i].at[out_rows(k), :], loc.at[8 + 2 * i + k])

    stage = None
    for m, s in ((m, s) for s in range(4) for m in (1, 2)):
        b = buf[m, s, 0]
        if stage is None and b.shape != (2, FC, HALF):
            stage = [b.at[0], b.at[1]] if b.shape[0] == 2 else [b.at[0, pl.ds(0, ROWS)], b.at[0, pl.ds(ROWS, ROWS)]]

    def finish(i, half):
        if half == 0:
            got(t_cp(i))
        acc, piece, dst = (yacc, dxacc)[i], (yl, dl)[i], (xs, gs)[i]

        def rows_of(q):
            return pl.ds(pl.multiple_of(half * HALF + q * ROWS, ROWS), ROWS)

        def fetch(q, k):
            return pltpu.make_async_copy(piece.at[rows_of(q), :], stage[k], isem.at[k])
        fetch(0, 0).start()

        def two(p, _):
            for k in (0, 1):
                q = 2 * p + k

                @pl.when(q + 1 < HALF // ROWS)
                def _():
                    fetch(q + 1, 1 - k).start()
                fetch(q, k).wait()
                rows = rows_of(q)
                dst[rows, :] = (acc[rows, :] + stage[k][...]).astype(BF16)
            return 0
        lax.fori_loop(0, HALF // ROWS // 2, two, 0)
        l_yo(i, half).start()

    def event(name):
        kind, a = name.rstrip("0123456789"), name.lstrip("abcdefghijklmnopqrstuvwxyz")
        n = int(a[0]) if a else 0
        hop_of = [int(q) for q in a[:3]] + [int(a[3]) if len(a) > 3 else None]
        if kind == "gwy":
            go(*wy(n))
        elif kind == "gwxo":
            go(*wx(n), *wp(n))
        elif kind == "gt":
            go(*ty(n), *tp(n))
            for cp in tl(n):
                cp.start()
        elif kind in ("gwxf", "gwzx", "gwz"):
            go(*{"gwxf": wxf, "gwzx": wzx, "gwz": wz}[kind](n))
        elif kind == "gh":
            go(*[q[0] for q in hop(*hop_of)])
        elif kind == "ga":
            go(*gives(n, int(a[1]), True))
        elif kind == "gyo":
            go(t_yo(n, int(a[1])))
        elif kind == "fw":
            got(*wy_in(n))
        elif kind == "fzx":
            got(*wx_in(n))
        elif kind == "fz":
            got(*(wz(n) if ROUTES[n] == "B" else wxf(n)))
        elif kind == "lw":
            if n % 2 == 0:
                s = n // 2
                got(*wzx(s), *(wxf(s) if ROUTES[s] == "B" else wz(s)), *wp(s))
            load_w(n, n % 2, True)
        elif kind == "ft":
            got(*ty(n))
            go(*tf(n))
            for cp in tl(n):
                cp.wait()
        elif kind == "fr":
            got(*tp(n), *tf(n))
        elif kind == "b":
            add_hop(*hop_of)
        elif kind == "cp":
            go(t_cp(0), t_cp(1))
            for i in (0, 1):
                for cp in tf(i):
                    cp.wait_send()
        elif kind == "fin":
            finish(n, int(a[1]))

    def zero(i, _):
        rows = pl.ds(pl.multiple_of(i * 64, 64), 64)
        yacc[rows, :] = jnp.zeros((64, HID), F32)
        dxacc[rows, :] = jnp.zeros((64, HID), F32)
        return 0
    plan = {n: list(v) for n, v in PLAN.items()}
    plan.setdefault(1, []).append("fr0")
    plan.setdefault(3, []).append("fr1")
    first = [q for q in range(len(plan[0])) if plan[0][q][0] != "g"][0]
    for name in plan[0][:first]:
        event(name)
    lax.fori_loop(0, TOK // 64, zero, 0)
    for name in plan[0][first:]:
        event(name)

    def tile(n, _):
        for at in sorted(plan):
            if 0 < at < NCH * NT:
                @pl.when(n == at)
                def _():
                    for name in plan[at]:
                        event(name)
        j, q = n // NT, n % NT
        slot = j % 2

        @pl.when(q == 0)
        def _():
            load_w(j, slot, False)
        w1, w2 = w1s.at[slot], w2s.at[slot]
        t = (q % 2) * 2 + q // 2
        rows = pl.ds(pl.multiple_of(t * TILE, TILE), TILE)
        xt, gt = xs[rows, :], gs[rows, :]
        u = dot(xt, w1[...], 1, 0)
        da = dot(gt, w2[...], 1, 1)
        cdf = 0.5 * (1.0 + lax.erf(u * INV_ROOT_TWO))
        act = (u * cdf).astype(BF16)
        du = (da * (cdf + u * jnp.exp(-0.5 * u * u) * INV_ROOT_TAU)).astype(BF16)
        yacc[rows, :] += dot(act, w2[...], 1, 0)
        dxacc[rows, :] += dot(du, w1[...], 1, 1)
        p2, p1 = dot(act, gt, 0, 0), dot(du, xt, 0, 0)

        @pl.when(q == 0)
        def _():
            d2[j] = p2
            d1[j] = p1

        @pl.when(q > 0)
        def _():
            d2[j] += p2
            d1[j] += p1
        return 0
    lax.fori_loop(0, NCH * NT, tile, 0)
    for name in plan[NCH * NT]:
        event(name)

    for s in range(4):
        for cp in wy(s) + wx(s) + wp(s) + wxf(s) + wzx(s) + wz(s):
            cp.wait_send()
        for m in (1, 2):
            for h in range(3):
                for cp, _, _ in hop(m, s, h):
                    cp.wait_send()
            for cp in gives(m, s, False) + gives(m, s, True):
                cp.wait_send()
                cp.wait_recv()
            for cp in stores(m, s):
                cp.wait()
    for i in (0, 1):
        for cp in ty(i) + tp(i) + [t_cp(i), t_yo(i, 0), t_yo(i, 1)]:
            cp.wait_send()
        for k in (0, 1):
            got(t_yo(i, k))
            l_yo(i, k).wait()


def fused(tok, grad, up, down):
    any_spec = pl.BlockSpec(memory_space=pl.ANY)
    vm, shape = pltpu.VMEM, jax.ShapeDtypeStruct
    land = [vm(dims, F32) for m in (1, 2) for s in range(4) for dims in hop_shapes(ORDERS[m][s])]
    dma = pltpu.SemaphoreType.DMA
    return pl.pallas_call(
        kernel,
        name="mlp_block",
        out_shape=(shape((TOK, HALF), BF16), shape((TOK, HALF), BF16), shape((2048, 256), F32), shape((1024, HALF), F32),
                   shape((TOK // 2, HID), F32), shape((TOK // 2, HID), F32),
                   shape((2, HID, HID), BF16), shape((2, HID, HID), BF16)),
        in_specs=[any_spec] * 4,
        out_specs=[any_spec] * 8,
        scratch_shapes=[
            vm((TOK, HID), BF16), vm((TOK, HID), BF16), vm((TOK, HID), F32), vm((TOK, HID), F32),
            vm((NCH, FC, HID), F32), vm((NCH, FC, HID), F32), vm((2, HID, FC), BF16), vm((2, FC, HID), BF16),
            dma((160,)), dma((160,)), dma((12,)), dma((2, 5)), dma((4,)), *land,
        ],
        compiler_params=pltpu.CompilerParams(collective_id=0, has_side_effects=True, vmem_limit_bytes=67_043_328),
    )(tok, grad, up, down)


def solution(mesh):
    act_spec = P(("depth", "row"), "col")
    wgt_spec = P("row", "col")

    def block(tok, up, down, grad):
        out = fused(tok, grad, up, down)
        return out[0], out[1], out[2].T, out[3]

    return jax.shard_map(block, mesh=mesh, in_specs=(act_spec, wgt_spec, wgt_spec, act_spec),
                         out_specs=(act_spec, act_spec, wgt_spec, wgt_spec), check_vma=False)
```

```python
import math
import jax
import jax.numpy as jnp
from jax import lax
from jax.experimental import pallas as pl
from jax.experimental.pallas import tpu as pltpu
from jax.sharding import PartitionSpec as P

INV_ROOT_TWO = 1.0 / math.sqrt(2.0)
INV_ROOT_TAU = 1.0 / math.sqrt(2.0 * math.pi)
MESH = pl.DeviceIdType.MESH
BF16, F32 = jnp.bfloat16, jnp.float32

TOK, HID, FC, NCH = 2048, 1024, 256, 8
HALF, TILE, ROWS = 512, 512, 128
NT = TOK // TILE
ROUTES = "BAAB"
ORDERS = {1: ("CBZ", "ZBC", "ZCB", "BCZ"),
          2: ("CBZ", "CBZ", "BZC", "BZC")}
PLAN = {
    0: ("gwxo0", "gwy1", "gwxo1", "gwy0", "gwxo2", "gt0", "fzx0", "fw1", "gwzx0", "gwxf1", "fzx1", "fw0",
        "gwz0", "gwzx1", "gwxo3", "fzx2", "gwzx2", "fz0", "gwxf0", "fz1", "gwz1", "gt1", "fzx3", "ft0",
        "gwzx3", "lw0", "lw1",),
    2: ("gwy2", "gwy3", "ft1",),
    4: ("fw2", "lw2", "gwxf2", "gh2000",),
    5: ("gh1000",),
    6: ("fw3", "gwz3",),
    8: ("fz2", "lw3", "gh2001", "gwz2",),
    9: ("gh1001",),
    10: ("fz3",),
    11: ("b2000",),
    12: ("b1000", "gh2100", "gh1100",),
    14: ("lw4", "gwxf3",),
    15: ("b2001",),
    16: ("lw5", "gh1101",),
    17: ("b1001", "gh101",),
    18: ("gh201",),
    19: ("b1100",),
    20: ("b2100", "gh1200",),
    21: ("lw6", "gh2101",),
    23: ("b1101",),
    24: ("lw7", "b101", "gh2200",),
    25: ("gh102",),
    26: ("b201", "gh111",),
    28: ("b1200",),
    29: ("b2101", "gh202",),
    32: ("cp", "gh2300", "gh1300", "b102", "b111", "gh1201", "b2200", "fin00", "b202", "fin01", "gh221",
        "gyo01", "fin10", "fin11", "b1201", "gh112", "b1300", "gh211", "gyo11", "b2300", "gh231", "b221",
        "b112", "ga11", "gh121", "gh222", "b231", "gh232", "b211", "gh212", "gh131", "gyo10", "b222",
        "ga22", "b121", "b232", "ga23", "b212", "gh122", "gyo00", "b131", "gh132", "b122", "ga12", "b132",),
}

def dot(a, b, ca, cb):
    return lax.dot_general(a, b, (((ca,), (cb,)), ((), ())), preferred_element_type=F32)


def hop_shapes(order):
    nb, rows, cols, shapes = 2, FC, HID, []
    for h, kind in enumerate(order):
        if kind == "B":
            nb = 1
        elif kind == "C":
            cols = HALF
        elif h < 2:
            rows = ROWS
        shapes.append((nb, rows, cols))
    return shapes


def kernel(x_in, g_in, up_in, down_in, y_out, dx_out, d1_out, d2_out, yl, dl, w1b, w2b,
           xs, gs, yacc, dxacc, d1, d2, w1s, w2s, send, recv, loc, wsem, isem, *land):
    z, y, r = lax.axis_index("depth"), lax.axis_index("col"), lax.axis_index("row")
    x, c = r // 2, r % 2
    r_x = (1 - x) * 2 + c
    r_c = r + 1 - 2 * c
    dev_c, dev_x, dev_xc = (z, y, r_c), (z, y, r_x), (z, y, (1 - x) * 2 + 1 - c)
    dev_y, dev_yc, dev_z, dev_zc = (z, 1 - y, r), (z, 1 - y, r_c), (1 - z, y, r), (1 - z, y, r_c)
    everything, lo, hi = slice(None), pl.ds(0, HALF), pl.ds(HALF, HALF)
    zrow = pl.ds(pl.multiple_of(z * ROWS, ROWS), ROWS)
    zoth = pl.ds(pl.multiple_of((1 - z) * ROWS, ROWS), ROWS)
    slots = {}

    def slot_of(name):
        return slots.setdefault(name, len(slots))

    def rc(name, src, dst, dev, arrives=None):
        return pltpu.make_async_remote_copy(
            src_ref=src, dst_ref=dst, send_sem=send.at[slot_of(name)],
            recv_sem=recv.at[slot_of(name if arrives is None else arrives)], device_id=dev, device_id_type=MESH)

    def go(*copies):
        for cp in copies:
            cp.start()

    def got(*copies):
        for cp in copies:
            cp.wait_recv()

    barrier = pltpu.get_barrier_semaphore()
    for dev in (dev_c, dev_x, dev_xc, dev_y, dev_yc, dev_z, dev_zc):
        pl.semaphore_signal(barrier, inc=1, device_id=dev, device_id_type=MESH)
    pl.semaphore_wait(barrier, 7)

    def chunk(q):
        return pl.ds(pl.multiple_of(q * FC, FC), FC)

    def up_cols(core, s):
        return pl.ds(pl.multiple_of(core * HID + s * FC, FC), FC)

    def part(xh, core, zi):
        return pl.ds(pl.multiple_of(xh * HALF + core * FC + zi * ROWS, ROWS), ROWS)

    def down_rows(s):
        return pl.ds(pl.multiple_of(s * FC + z * ROWS, ROWS), ROWS)

    def by_core(name, s, core, src, dst, dev):
        base = slot_of(f"{name}{s}0")
        slot_of(f"{name}{s}1")
        return pltpu.make_async_remote_copy(src_ref=src, dst_ref=dst, send_sem=send.at[base + core],
                                            recv_sem=recv.at[base + c], device_id=dev, device_id_type=MESH)

    def by_core_in(name, s, core, like):
        base = slot_of(f"{name}{s}0")
        slot_of(f"{name}{s}1")
        return pltpu.make_async_remote_copy(src_ref=like, dst_ref=like, send_sem=send.at[base + core],
                                            recv_sem=recv.at[base + core], device_id=dev_c, device_id_type=MESH)

    def wy(s):
        two = [by_core("wy", s, q, up_in.at[zrow, up_cols(q, s)], w1b.at[y, part(0, c, z), chunk(s)], (z, 1 - y, x * 2 + q))
               for q in (0, 1)]
        return two + [wy_down(s)]

    def wy_down(s):
        return rc(f"wY{s}", down_in.at[down_rows(s), :], w2b.at[x, down_rows(s), hi], dev_y)

    def wy_in(s):
        return [by_core_in("wy", s, q, w1b.at[1 - y, part(0, q, z), chunk(s)]) for q in (0, 1)] + [wy_down(s)]

    def wx(s):
        two = [by_core("wx", s, q, up_in.at[zrow, up_cols(q, s)], w1b.at[y, part(1, c, z), chunk(s)],
                       (z, y, (1 - x) * 2 + q)) for q in (0, 1)]
        return two + [wx_down(s)]

    def wx_down(s):
        return rc(f"wX{s}", down_in.at[down_rows(s), :], w2b.at[x, down_rows(s), lo], dev_x)

    def wx_in(s):
        return [by_core_in("wx", s, q, w1b.at[y, part(1, q, z), chunk(s)]) for q in (0, 1)] + [wx_down(s)]

    def wp(s):
        return [rc(f"wp{s}", up_in.at[:, up_cols(1 - c, s)], w1b.at[y, chunk(c), chunk(s)], dev_c)]

    def wxf(s):
        if ROUTES[s] == "B":
            both = w2b.at[x, chunk(s), hi]
            return [rc(f"wf{s}0", w1b.at[1 - y, lo, chunk(s)], w1b.at[1 - y, hi, chunk(s)], dev_x),
                    rc(f"wF{s}", both, both, dev_x)]
        two = [rc(f"wf{s}{q}", w1b.at[1 - y, part(0, q, z), chunk(s)], w1b.at[1 - y, part(1, q, z), chunk(s)], dev_x)
               for q in (0, 1)]
        both = w2b.at[x, down_rows(s), hi]
        return two + [rc(f"wF{s}", both, both, dev_x)]

    def same_z(name, ref):
        return rc(name, ref, ref, dev_z)

    def wzx(s):
        return [same_z(f"wzx{s}{q}", w1b.at[y, part(1, q, z), chunk(s)]) for q in (0, 1)] + [
            same_z(f"wzX{s}", w2b.at[1 - x, down_rows(s), lo])]

    def wz(s):
        if ROUTES[s] == "B":
            return [same_z(f"wz{s}0{q}", w1b.at[1 - y, part(0, q, z), chunk(s)]) for q in (0, 1)] + [
                same_z(f"wZ{s}0", w2b.at[x, down_rows(s), hi])]
        return [same_z(f"wz{s}{h}{q}", w1b.at[1 - y, part(h, q, z), chunk(s)]) for h in (0, 1) for q in (0, 1)] + [
            same_z(f"wZ{s}{i}", w2b.at[(x, 1 - x)[i], down_rows(s), hi]) for i in (0, 1)]

    def load_w(j, slot, start):
        s, b = j // 2, j % 2

        def cp(src, dst, k):
            copy = pltpu.make_async_copy(src, dst, wsem.at[slot, k])
            copy.start() if start else copy.wait()
        v1, v2 = w1s.at[slot], w2s.at[slot]
        if start:
            @pl.when(b == y)
            def _():
                cp(up_in.at[:, up_cols(c, s)], v1.at[chunk(c), :], 0)

            @pl.when(b != y)
            def _():
                cp(w1b.at[b, chunk(c), chunk(s)], v1.at[chunk(c), :], 0)

            @pl.when(b == x)
            def _():
                cp(down_in.at[chunk(s), :], v2.at[:, lo], 3)

            @pl.when(b != x)
            def _():
                cp(w2b.at[b, chunk(s), lo], v2.at[:, lo], 3)
        else:
            cp(up_in.at[:, up_cols(c, s)], v1.at[chunk(c), :], 0)
            cp(down_in.at[chunk(s), :], v2.at[:, lo], 3)
        cp(w1b.at[b, chunk(1 - c), chunk(s)], v1.at[chunk(1 - c), :], 1)
        cp(w1b.at[b, hi, chunk(s)], v1.at[hi, :], 2)
        cp(w2b.at[b, chunk(s), hi], v2.at[:, hi], 4)

    own_cols = (pl.ds(pl.multiple_of(jnp.where(x == y, 0, HALF), HALF), HALF), lo)
    far_cols = (pl.ds(pl.multiple_of(jnp.where(x == y, HALF, 0), HALF), HALF), hi)
    ins, tok = (x_in, g_in), (xs, gs)

    def tok_at(base, i):
        return pl.ds(pl.multiple_of(base * (TOK // 2) + i * TILE, TILE), TILE)

    def ty(i):
        return [rc(f"ty{i}{k}", ins[k].at[tok_at(1 - y, i), :], tok[k].at[tok_at(0, i), (own_cols[0], hi)[k]], dev_y)
                for k in (0, 1)]

    def tp(i):
        return [rc(f"tp{i}{k}", ins[k].at[tok_at(y, i), :], tok[k].at[tok_at(1, i), own_cols[k]], dev_c) for k in (0, 1)]

    def tf(i):
        return [rc(f"tf{i}{k}", tok[k].at[tok_at(0, i), far_cols[k]], tok[k].at[tok_at(1, i), far_cols[k]], dev_c)
                for k in (0, 1)]

    def tl(i):
        return [pltpu.make_async_copy(ins[k].at[tok_at(y, i), :], tok[k].at[tok_at(0, i), own_cols[k]],
                                      isem.at[2 * i + k]) for k in (0, 1)]

    parts = {1: d1, 2: d2}
    buf = {(m, s, h): land[(m - 1) * 12 + s * 3 + h] for m in (1, 2) for s in range(4) for h in range(3)}
    keep_block = {1: y, 2: x}
    dev_of = {(1, "C"): dev_x, (1, "B"): dev_y, (1, "Z"): dev_z, (2, "C"): dev_y, (2, "B"): dev_x, (2, "Z"): dev_z}

    def live(m, s, h):
        blocks, rows, cols = [2 * s, 2 * s + 1], everything, everything
        for kind in ORDERS[m][s][:h]:
            if kind == "B":
                blocks = [2 * s + keep_block[m]]
            elif kind == "C":
                cols = lo
            else:
                rows = zrow
        return blocks, rows, cols

    def hop(m, s, h, only=None):
        kind = ORDERS[m][s][h]
        blocks, rows, cols = live(m, s, h)
        d, b, dev = parts[m], buf[m, s, h], dev_of[m, kind]
        if kind == "B":
            ends = [(d.at[2 * s + 1 - keep_block[m], rows, cols], (2 * s + keep_block[m], rows, cols))]
        elif kind == "C":
            ends = [(d.at[q, rows, hi], (q, rows, lo)) for q in blocks]
        elif h < 2:
            ends = [(d.at[q, zoth, cols], (q, zrow, cols)) for q in blocks]
        else:
            ends = [(d.at[q, rows, cols], (q, rows, cols)) for q in blocks]
        return [(rc(f"h{m}{s}{h}{i}", src, b.at[i], dev), b.at[i], into)
                for i, (src, into) in enumerate(ends) if only is None or i == only]

    def add_hop(m, s, h, only=None):
        for cp, landed, (q, rows, cols) in hop(m, s, h, only):
            got(cp)
            if h < 2:
                parts[m][q, rows, cols] += landed[...]
            else:
                landed[...] += parts[m][q, rows, cols]
        if h == 2:
            go(*gives(m, s, False))
            for cp in stores(m, s):
                cp.start()

    def fin_rows(m, s, other=False):
        split = ORDERS[m][s][2] != "Z"
        base = s * FC + (c * HID if m == 1 else 0)
        if split:
            base = base + ((1 - z) if other else z) * ROWS
        return pl.ds(pl.multiple_of(base, ROWS), ROWS if split else FC)

    def cols_c(q):
        return pl.ds(pl.multiple_of(q * 256, 256), 256)

    def gives(m, s, far):
        b, split = buf[m, s, 2], ORDERS[m][s][2] != "Z"
        rows = fin_rows(m, s)
        if far and not split or m == 2 and not far:
            return []
        if m == 2:
            return [rc(f"a2{s}", b.at[0], d2_out.at[rows, :], dev_z)]
        if not far:
            return [rc(f"c1{s}", b.at[0, :, cols_c(1 - c)], d1_out.at[rows, :], dev_c)]
        return [rc(f"a1{s}", b.at[0, :, cols_c(c)], d1_out.at[rows, :], dev_z),
                rc(f"k1{s}", b.at[0, :, cols_c(1 - c)], d1_out.at[rows, :], dev_zc)]

    def stores(m, s):
        b = buf[m, s, 2]
        if m == 2:
            return [pltpu.make_async_copy(b.at[0], d2_out.at[fin_rows(m, s), :], loc.at[4 + s])]
        return [pltpu.make_async_copy(b.at[0, :, cols_c(c)], d1_out.at[fin_rows(m, s), :], loc.at[s])]

    mine, theirs = pl.ds(0, TOK // 2), pl.ds(TOK // 2, TOK // 2)

    def t_cp(i):
        return rc(f"cp{i}", (yacc, dxacc)[i].at[theirs, :], (yl, dl)[i], dev_c)

    def out_rows(k):
        return pl.ds(pl.multiple_of(y * (TOK // 2) + k * HALF, HALF), HALF)

    def t_yo(i, k):
        return rc(f"yo{i}{k}", (xs, gs)[i].at[pl.ds(k * HALF, HALF), (hi, far_cols[0])[i]],
                  (y_out, dx_out)[i].at[out_rows(k), :], dev_y)

    def l_yo(i, k):
        return pltpu.make_async_copy((xs, gs)[i].at[pl.ds(k * HALF, HALF), (lo, own_cols[0])[i]],
                                     (y_out, dx_out)[i].at[out_rows(k), :], loc.at[8 + 2 * i + k])

    stage = None
    for m, s in ((m, s) for s in range(4) for m in (1, 2)):
        b = buf[m, s, 0]
        if stage is None and b.shape != (2, FC, HALF):
            stage = [b.at[0], b.at[1]] if b.shape[0] == 2 else [b.at[0, pl.ds(0, ROWS)], b.at[0, pl.ds(ROWS, ROWS)]]

    def finish(i, half):
        if half == 0:
            got(t_cp(i))
        acc, piece, dst = (yacc, dxacc)[i], (yl, dl)[i], (xs, gs)[i]

        def rows_of(q):
            return pl.ds(pl.multiple_of(half * HALF + q * ROWS, ROWS), ROWS)

        def fetch(q, k):
            return pltpu.make_async_copy(piece.at[rows_of(q), :], stage[k], isem.at[k])
        fetch(0, 0).start()

        def two(p, _):
            for k in (0, 1):
                q = 2 * p + k

                @pl.when(q + 1 < HALF // ROWS)
                def _():
                    fetch(q + 1, 1 - k).start()
                fetch(q, k).wait()
                rows = rows_of(q)
                dst[rows, :] = (acc[rows, :] + stage[k][...]).astype(BF16)
            return 0
        lax.fori_loop(0, HALF // ROWS // 2, two, 0)
        l_yo(i, half).start()

    def event(name):
        kind, a = name.rstrip("0123456789"), name.lstrip("abcdefghijklmnopqrstuvwxyz")
        n = int(a[0]) if a else 0
        hop_of = [int(q) for q in a[:3]] + [int(a[3]) if len(a) > 3 else None]
        if kind == "gwy":
            go(*wy(n))
        elif kind == "gwxo":
            go(*wx(n), *wp(n))
        elif kind == "gt":
            go(*ty(n), *tp(n))
            for cp in tl(n):
                cp.start()
        elif kind in ("gwxf", "gwzx", "gwz"):
            go(*{"gwxf": wxf, "gwzx": wzx, "gwz": wz}[kind](n))
        elif kind == "gh":
            go(*[q[0] for q in hop(*hop_of)])
        elif kind == "ga":
            go(*gives(n, int(a[1]), True))
        elif kind == "gyo":
            go(t_yo(n, int(a[1])))
        elif kind == "fw":
            got(*wy_in(n))
        elif kind == "fzx":
            got(*wx_in(n))
        elif kind == "fz":
            got(*(wz(n) if ROUTES[n] == "B" else wxf(n)))
        elif kind == "lw":
            if n % 2 == 0:
                s = n // 2
                got(*wzx(s), *(wxf(s) if ROUTES[s] == "B" else wz(s)), *wp(s))
            load_w(n, n % 2, True)
        elif kind == "ft":
            got(*ty(n))
            go(*tf(n))
            for cp in tl(n):
                cp.wait()
        elif kind == "fr":
            got(*tp(n), *tf(n))
        elif kind == "b":
            add_hop(*hop_of)
        elif kind == "cp":
            go(t_cp(0), t_cp(1))
            for i in (0, 1):
                for cp in tf(i):
                    cp.wait_send()
        elif kind == "fin":
            finish(n, int(a[1]))

    def zero(i, _):
        rows = pl.ds(pl.multiple_of(i * 64, 64), 64)
        yacc[rows, :] = jnp.zeros((64, HID), F32)
        dxacc[rows, :] = jnp.zeros((64, HID), F32)
        return 0
    plan = {n: list(v) for n, v in PLAN.items()}
    plan.setdefault(1, []).append("fr0")
    plan.setdefault(3, []).append("fr1")
    first = [q for q in range(len(plan[0])) if plan[0][q][0] != "g"][0]
    for name in plan[0][:first]:
        event(name)
    lax.fori_loop(0, TOK // 64, zero, 0)
    for name in plan[0][first:]:
        event(name)

    def tile(n, _):
        for at in sorted(plan):
            if 0 < at < NCH * NT:
                @pl.when(n == at)
                def _():
                    for name in plan[at]:
                        event(name)
        j, q = n // NT, n % NT
        slot = j % 2

        @pl.when(q == 0)
        def _():
            load_w(j, slot, False)
        w1, w2 = w1s.at[slot], w2s.at[slot]
        t = (q % 2) * 2 + q // 2
        rows = pl.ds(pl.multiple_of(t * TILE, TILE), TILE)
        xt, gt = xs[rows, :], gs[rows, :]
        u = dot(xt, w1[...], 1, 0)
        da = dot(gt, w2[...], 1, 1)
        cdf = 0.5 * (1.0 + lax.erf(u * INV_ROOT_TWO))
        act = (u * cdf).astype(BF16)
        du = (da * (cdf + u * jnp.exp(-0.5 * u * u) * INV_ROOT_TAU)).astype(BF16)
        yacc[rows, :] += dot(act, w2[...], 1, 0)
        dxacc[rows, :] += dot(du, w1[...], 1, 1)
        p2, p1 = dot(act, gt, 0, 0), dot(du, xt, 0, 0)

        @pl.when(q == 0)
        def _():
            d2[j] = p2
            d1[j] = p1

        @pl.when(q > 0)
        def _():
            d2[j] += p2
            d1[j] += p1
        return 0
    lax.fori_loop(0, NCH * NT, tile, 0)
    for name in plan[NCH * NT]:
        event(name)

    for s in range(4):
        for cp in wy(s) + wx(s) + wp(s) + wxf(s) + wzx(s) + wz(s):
            cp.wait_send()
        for m in (1, 2):
            for h in range(3):
                for cp, _, _ in hop(m, s, h):
                    cp.wait_send()
            for cp in gives(m, s, False) + gives(m, s, True):
                cp.wait_send()
                cp.wait_recv()
            for cp in stores(m, s):
                cp.wait()
    for i in (0, 1):
        for cp in ty(i) + tp(i) + [t_cp(i), t_yo(i, 0), t_yo(i, 1)]:
            cp.wait_send()
        for k in (0, 1):
            got(t_yo(i, k))
            l_yo(i, k).wait()


def fused(tok, grad, up, down):
    any_spec = pl.BlockSpec(memory_space=pl.ANY)
    vm, shape = pltpu.VMEM, jax.ShapeDtypeStruct
    land = [vm(dims, F32) for m in (1, 2) for s in range(4) for dims in hop_shapes(ORDERS[m][s])]
    dma = pltpu.SemaphoreType.DMA
    return pl.pallas_call(
        kernel,
        name="mlp_block",
        out_shape=(shape((TOK, HALF), BF16), shape((TOK, HALF), BF16), shape((2048, 256), F32), shape((1024, HALF), F32),
                   shape((TOK // 2, HID), F32), shape((TOK // 2, HID), F32),
                   shape((2, HID, HID), BF16), shape((2, HID, HID), BF16)),
        in_specs=[any_spec] * 4,
        out_specs=[any_spec] * 8,
        scratch_shapes=[
            vm((TOK, HID), BF16), vm((TOK, HID), BF16), vm((TOK, HID), F32), vm((TOK, HID), F32),
            vm((NCH, FC, HID), F32), vm((NCH, FC, HID), F32), vm((2, HID, FC), BF16), vm((2, FC, HID), BF16),
            dma((160,)), dma((160,)), dma((12,)), dma((2, 5)), dma((4,)), *land,
        ],
        compiler_params=pltpu.CompilerParams(collective_id=0, has_side_effects=True, vmem_limit_bytes=67_043_328),
    )(tok, grad, up, down)


def settle_kernel(y_in, dx_in, d1_in, d2_in, y_ref, dx_ref, d1_ref, d2_ref):
    y_ref[...] = y_in[...]
    dx_ref[...] = dx_in[...]
    d1_ref[...] = d1_in[...].T
    d2_ref[...] = d2_in[...]


def settle(y, dx, d1t, d2):
    steps = 2
    shape = jax.ShapeDtypeStruct

    def rows(n, cols):
        return pl.BlockSpec((n // steps, cols), lambda i: (i, 0))
    return pl.pallas_call(
        settle_kernel,
        name="settle",
        grid=(steps,),
        out_shape=(shape(y.shape, BF16), shape(dx.shape, BF16), shape(d1t.shape[::-1], F32), shape(d2.shape, F32)),
        in_specs=[rows(TOK, HALF), rows(TOK, HALF), rows(2048, 256), rows(1024, HALF)],
        out_specs=[rows(TOK, HALF), rows(TOK, HALF), pl.BlockSpec((256, 2048 // steps), lambda i: (0, i)), rows(1024, HALF)],
    )(y, dx, d1t, d2)


def solution(mesh):
    act_spec = P(("depth", "row"), "col")
    wgt_spec = P("row", "col")

    def block(tok, up, down, grad):
        return settle(*fused(tok, grad, up, down)[:4])

    return jax.shard_map(block, mesh=mesh, in_specs=(act_spec, wgt_spec, wgt_spec, act_spec),
                         out_specs=(act_spec, act_spec, wgt_spec, wgt_spec), check_vma=False)
```

```python
import math
import jax
import jax.numpy as jnp
from jax import lax
from jax.experimental import pallas as pl
from jax.experimental.pallas import tpu as pltpu
from jax.sharding import PartitionSpec as P

INV_ROOT_TWO = 1.0 / math.sqrt(2.0)
INV_ROOT_TAU = 1.0 / math.sqrt(2.0 * math.pi)
MESH = pl.DeviceIdType.MESH
BF16, F32 = jnp.bfloat16, jnp.float32

TOK, HID, FC, NCH = 2048, 1024, 256, 8
HALF, TILE, ROWS, SMALL = 512, 512, 128, 64
NT = TOK // TILE
ROUTES = "BAAB"
ORDERS = {1: ("ZBC", "CBZ", "BZC", "CBZ", "CBZ", "BZC", "ZCB", "CZB"),
          2: ("CZB", "CBZ", "BZC", "ZBC", "BZC", "CZB", "BCZ", "BCZ")}
PLAN = {
    0: ("gwxo0", "gwy1", "gwxo1", "gwy0", "gwxo2", "gt0", "fzx0", "fw1", "gwzx0", "gwxf1", "fzx1", "fw0",
        "gwz0", "gwzx1", "gwxo3", "fzx2", "gwzx2", "fz0", "gwxf0", "fz1", "gwz1", "gt1", "fzx3", "ft0",
        "gwzx3", "lw0", "lw1",),
    2: ("gwy2", "gwy3", "ft1",),
    4: ("fw2", "lw2", "gwxf2", "gh2000", "gh1000",),
    5: ("gh1100", "gh2100",),
    6: ("fw3", "gwz3",),
    8: ("fz2", "lw3", "b1000", "b2000", "gh1101", "gh2101", "gwz2",),
    10: ("fz3", "b1100", "gwxf3", "gh2001",),
    11: ("b2100",),
    12: ("b1101", "gh111", "gh2300",),
    13: ("b2101",),
    14: ("gh1300", "gh1001",),
    15: ("lw4", "b2001",),
    16: ("lw5", "gh1301", "gh1200", "gh2301", "b2300",),
    17: ("b111",),
    18: ("gh2200", "gh112",),
    19: ("b1300", "b1001", "gh101",),
    20: ("lw6", "gh201",),
    21: ("b1301", "b2301", "gh131",),
    22: ("b1200", "gh1400", "gh121",),
    23: ("b112", "gh2500",),
    24: ("lw7", "b101",),
    25: ("b2200", "b201", "gh2400", "gh1500", "gh221",),
    26: ("b131",),
    27: ("gh132",),
    28: ("b1400", "b121", "b2500",),
    29: ("gh1401", "gh1600",),
    30: ("b221", "gh222",),
    31: ("gh1700", "gh2501",),
    32: ("cp", "b2400", "b132", "gh241", "b1500", "gh2600", "gh1601", "b222", "b1401", "b1600", "gh141",
        "ga22", "b2501", "b1700", "b241", "gh242", "fin00", "gyo00", "gh251", "fin01", "b141", "gh2700",
        "b1601", "gh142", "b242", "fin10", "fin11", "b2600", "gh261", "ga24", "b251", "gh252", "gh151",
        "gyo10", "gh1701", "b142", "b2700", "gh161", "b261", "gh262", "b252", "ga25", "gh271", "b151",
        "gh152", "b1701", "gh171", "gh122", "gyo01", "b262", "gh231", "b161", "b152", "ga15", "gh102",
        "b271", "gh272", "b122", "b171", "gh202", "ga12", "gh162", "gh211", "gh172", "b231", "gh232",
        "b102", "b272", "ga10", "gyo11", "b202", "ga20", "b162", "ga16", "b172", "ga17", "b211", "gh212",
        "b232", "ga23", "b212",),
}

def dot(a, b, ca, cb):
    return lax.dot_general(a, b, (((ca,), (cb,)), ((), ())), preferred_element_type=F32)


def hop_shapes(order):
    nb, rows, cols, shapes = 2, ROWS, HID, []
    for h, kind in enumerate(order):
        if kind == "B":
            nb = 1
        elif kind == "C":
            cols = HALF
        elif h < 2:
            rows = ROWS // 2
        shapes.append((nb, rows, cols))
    return shapes


def kernel(x_in, g_in, up_in, down_in, y_out, dx_out, d1_out, d2_out, yl, dl, w1b, w2b,
           xs, gs, yacc, dxacc, d1, d2, w1s, w2s, send, recv, loc, wsem, isem, *land):
    z, y, r = lax.axis_index("depth"), lax.axis_index("col"), lax.axis_index("row")
    x, c = r // 2, r % 2
    r_x = (1 - x) * 2 + c
    r_c = r + 1 - 2 * c
    dev_c, dev_x, dev_xc = (z, y, r_c), (z, y, r_x), (z, y, (1 - x) * 2 + 1 - c)
    dev_y, dev_yc, dev_z, dev_zc = (z, 1 - y, r), (z, 1 - y, r_c), (1 - z, y, r), (1 - z, y, r_c)
    everything, lo, hi = slice(None), pl.ds(0, HALF), pl.ds(HALF, HALF)
    zrow = pl.ds(pl.multiple_of(z * ROWS, ROWS), ROWS)
    zoth = pl.ds(pl.multiple_of((1 - z) * ROWS, ROWS), ROWS)
    slots = {}

    def slot_of(name):
        return slots.setdefault(name, len(slots))

    def rc(name, src, dst, dev, arrives=None):
        return pltpu.make_async_remote_copy(
            src_ref=src, dst_ref=dst, send_sem=send.at[slot_of(name)],
            recv_sem=recv.at[slot_of(name if arrives is None else arrives)], device_id=dev, device_id_type=MESH)

    def go(*copies):
        for cp in copies:
            cp.start()

    def got(*copies):
        for cp in copies:
            cp.wait_recv()

    barrier = pltpu.get_barrier_semaphore()
    for dev in (dev_c, dev_x, dev_xc, dev_y, dev_yc, dev_z, dev_zc):
        pl.semaphore_signal(barrier, inc=1, device_id=dev, device_id_type=MESH)
    pl.semaphore_wait(barrier, 7)

    def chunk(q):
        return pl.ds(pl.multiple_of(q * FC, FC), FC)

    def up_cols(core, s):
        return pl.ds(pl.multiple_of(core * HID + s * FC, FC), FC)

    def part(xh, core, zi):
        return pl.ds(pl.multiple_of(xh * HALF + core * FC + zi * ROWS, ROWS), ROWS)

    def down_rows(s):
        return pl.ds(pl.multiple_of(s * FC + z * ROWS, ROWS), ROWS)

    def by_core(name, s, core, src, dst, dev):
        base = slot_of(f"{name}{s}0")
        slot_of(f"{name}{s}1")
        return pltpu.make_async_remote_copy(src_ref=src, dst_ref=dst, send_sem=send.at[base + core],
                                            recv_sem=recv.at[base + c], device_id=dev, device_id_type=MESH)

    def by_core_in(name, s, core, like):
        base = slot_of(f"{name}{s}0")
        slot_of(f"{name}{s}1")
        return pltpu.make_async_remote_copy(src_ref=like, dst_ref=like, send_sem=send.at[base + core],
                                            recv_sem=recv.at[base + core], device_id=dev_c, device_id_type=MESH)

    def wy(s):
        two = [by_core("wy", s, q, up_in.at[zrow, up_cols(q, s)], w1b.at[y, part(0, c, z), chunk(s)], (z, 1 - y, x * 2 + q))
               for q in (0, 1)]
        return two + [wy_down(s)]

    def wy_down(s):
        return rc(f"wY{s}", down_in.at[down_rows(s), :], w2b.at[x, down_rows(s), hi], dev_y)

    def wy_in(s):
        return [by_core_in("wy", s, q, w1b.at[1 - y, part(0, q, z), chunk(s)]) for q in (0, 1)] + [wy_down(s)]

    def wx(s):
        two = [by_core("wx", s, q, up_in.at[zrow, up_cols(q, s)], w1b.at[y, part(1, c, z), chunk(s)],
                       (z, y, (1 - x) * 2 + q)) for q in (0, 1)]
        return two + [wx_down(s)]

    def wx_down(s):
        return rc(f"wX{s}", down_in.at[down_rows(s), :], w2b.at[x, down_rows(s), lo], dev_x)

    def wx_in(s):
        return [by_core_in("wx", s, q, w1b.at[y, part(1, q, z), chunk(s)]) for q in (0, 1)] + [wx_down(s)]

    def wp(s):
        return [rc(f"wp{s}", up_in.at[:, up_cols(1 - c, s)], w1b.at[y, chunk(c), chunk(s)], dev_c)]

    def wxf(s):
        if ROUTES[s] == "B":
            both = w2b.at[x, chunk(s), hi]
            return [rc(f"wf{s}0", w1b.at[1 - y, lo, chunk(s)], w1b.at[1 - y, hi, chunk(s)], dev_x),
                    rc(f"wF{s}", both, both, dev_x)]
        two = [rc(f"wf{s}{q}", w1b.at[1 - y, part(0, q, z), chunk(s)], w1b.at[1 - y, part(1, q, z), chunk(s)], dev_x)
               for q in (0, 1)]
        both = w2b.at[x, down_rows(s), hi]
        return two + [rc(f"wF{s}", both, both, dev_x)]

    def same_z(name, ref):
        return rc(name, ref, ref, dev_z)

    def wzx(s):
        return [same_z(f"wzx{s}{q}", w1b.at[y, part(1, q, z), chunk(s)]) for q in (0, 1)] + [
            same_z(f"wzX{s}", w2b.at[1 - x, down_rows(s), lo])]

    def wz(s):
        if ROUTES[s] == "B":
            return [same_z(f"wz{s}0{q}", w1b.at[1 - y, part(0, q, z), chunk(s)]) for q in (0, 1)] + [
                same_z(f"wZ{s}0", w2b.at[x, down_rows(s), hi])]
        return [same_z(f"wz{s}{h}{q}", w1b.at[1 - y, part(h, q, z), chunk(s)]) for h in (0, 1) for q in (0, 1)] + [
            same_z(f"wZ{s}{i}", w2b.at[(x, 1 - x)[i], down_rows(s), hi]) for i in (0, 1)]

    def load_w(j, slot, start):
        s, b = j // 2, j % 2

        def cp(src, dst, k):
            copy = pltpu.make_async_copy(src, dst, wsem.at[slot, k])
            copy.start() if start else copy.wait()
        v1, v2 = w1s.at[slot], w2s.at[slot]
        if start:
            @pl.when(b == y)
            def _():
                cp(up_in.at[:, up_cols(c, s)], v1.at[chunk(c), :], 0)

            @pl.when(b != y)
            def _():
                cp(w1b.at[b, chunk(c), chunk(s)], v1.at[chunk(c), :], 0)

            @pl.when(b == x)
            def _():
                cp(down_in.at[chunk(s), :], v2.at[:, lo], 3)

            @pl.when(b != x)
            def _():
                cp(w2b.at[b, chunk(s), lo], v2.at[:, lo], 3)
        else:
            cp(up_in.at[:, up_cols(c, s)], v1.at[chunk(c), :], 0)
            cp(down_in.at[chunk(s), :], v2.at[:, lo], 3)
        cp(w1b.at[b, chunk(1 - c), chunk(s)], v1.at[chunk(1 - c), :], 1)
        cp(w1b.at[b, hi, chunk(s)], v1.at[hi, :], 2)
        cp(w2b.at[b, chunk(s), hi], v2.at[:, hi], 4)

    own_cols = (pl.ds(pl.multiple_of(jnp.where(x == y, 0, HALF), HALF), HALF), lo)
    far_cols = (pl.ds(pl.multiple_of(jnp.where(x == y, HALF, 0), HALF), HALF), hi)
    ins, tok = (x_in, g_in), (xs, gs)

    def tok_at(base, i):
        return pl.ds(pl.multiple_of(base * (TOK // 2) + i * TILE, TILE), TILE)

    def ty(i):
        return [rc(f"ty{i}{k}", ins[k].at[tok_at(1 - y, i), :], tok[k].at[tok_at(0, i), (own_cols[0], hi)[k]], dev_y)
                for k in (0, 1)]

    def tp(i):
        return [rc(f"tp{i}{k}", ins[k].at[tok_at(y, i), :], tok[k].at[tok_at(1, i), own_cols[k]], dev_c) for k in (0, 1)]

    def tf(i):
        return [rc(f"tf{i}{k}", tok[k].at[tok_at(0, i), far_cols[k]], tok[k].at[tok_at(1, i), far_cols[k]], dev_c)
                for k in (0, 1)]

    def tl(i):
        return [pltpu.make_async_copy(ins[k].at[tok_at(y, i), :], tok[k].at[tok_at(0, i), own_cols[k]],
                                      isem.at[2 * i + k]) for k in (0, 1)]

    parts = {1: d1, 2: d2}
    buf = {(m, u, h): land[(m - 1) * 24 + u * 3 + h] for m in (1, 2) for u in range(8) for h in range(3)}
    keep_block = {1: y, 2: x}
    dev_of = {(1, "C"): dev_x, (1, "B"): dev_y, (1, "Z"): dev_z, (2, "C"): dev_y, (2, "B"): dev_x, (2, "Z"): dev_z}

    def z_rows(u, zi):
        return pl.ds(pl.multiple_of(u % 2 * ROWS + zi * (ROWS // 2), ROWS // 2), ROWS // 2)

    def live(m, u, h):
        first = u // 2 * 2
        blocks, rows, cols = [first, first + 1], pl.ds(u % 2 * ROWS, ROWS), everything
        for kind in ORDERS[m][u][:h]:
            if kind == "B":
                blocks = [first + keep_block[m]]
            elif kind == "C":
                cols = lo
            else:
                rows = z_rows(u, z)
        return blocks, rows, cols

    def hop(m, u, h, only=None):
        kind = ORDERS[m][u][h]
        blocks, rows, cols = live(m, u, h)
        d, b, dev, first = parts[m], buf[m, u, h], dev_of[m, kind], u // 2 * 2
        if kind == "B":
            ends = [(d.at[first + 1 - keep_block[m], rows, cols], (first + keep_block[m], rows, cols))]
        elif kind == "C":
            ends = [(d.at[q, rows, hi], (q, rows, lo)) for q in blocks]
        elif h < 2:
            ends = [(d.at[q, z_rows(u, 1 - z), cols], (q, z_rows(u, z), cols)) for q in blocks]
        else:
            ends = [(d.at[q, rows, cols], (q, rows, cols)) for q in blocks]
        return [(rc(f"h{m}{u}{h}{i}", src, b.at[i], dev), b.at[i], into)
                for i, (src, into) in enumerate(ends) if only is None or i == only]

    def add_hop(m, s, h, only=None):
        for cp, landed, (q, rows, cols) in hop(m, s, h, only):
            got(cp)
            if h < 2:
                parts[m][q, rows, cols] += landed[...]
            else:
                landed[...] += parts[m][q, rows, cols]
        if h == 2:
            go(*gives(m, s, False))
            for cp in stores(m, s):
                cp.start()

    def fin_rows(m, u):
        split = ORDERS[m][u][2] != "Z"
        base = u * ROWS + (c * HID if m == 1 else 0)
        if split:
            base = base + z * (ROWS // 2)
        return pl.ds(pl.multiple_of(base, ROWS // 2), ROWS // 2 if split else ROWS)

    def cols_c(q):
        return pl.ds(pl.multiple_of(q * 256, 256), 256)

    def gives(m, s, far):
        b, split = buf[m, s, 2], ORDERS[m][s][2] != "Z"
        rows = fin_rows(m, s)
        if far and not split or m == 2 and not far:
            return []
        if m == 2:
            return [rc(f"a2{s}", b.at[0], d2_out.at[rows, :], dev_z)]
        if not far:
            return [rc(f"c1{s}", b.at[0, :, cols_c(1 - c)], d1_out.at[rows, :], dev_c)]
        return [rc(f"a1{s}", b.at[0, :, cols_c(c)], d1_out.at[rows, :], dev_z),
                rc(f"k1{s}", b.at[0, :, cols_c(1 - c)], d1_out.at[rows, :], dev_zc)]

    def stores(m, s):
        b = buf[m, s, 2]
        if m == 2:
            return [pltpu.make_async_copy(b.at[0], d2_out.at[fin_rows(m, s), :], loc.at[8 + s])]
        return [pltpu.make_async_copy(b.at[0, :, cols_c(c)], d1_out.at[fin_rows(m, s), :], loc.at[s])]

    mine, theirs = pl.ds(0, TOK // 2), pl.ds(TOK // 2, TOK // 2)

    def t_cp(i):
        return rc(f"cp{i}", (yacc, dxacc)[i].at[theirs, :], (yl, dl)[i], dev_c)

    def out_rows(k):
        return pl.ds(pl.multiple_of(y * (TOK // 2) + k * HALF, HALF), HALF)

    def t_yo(i, k):
        return rc(f"yo{i}{k}", (xs, gs)[i].at[pl.ds(k * HALF, HALF), (hi, far_cols[0])[i]],
                  (y_out, dx_out)[i].at[out_rows(k), :], dev_y)

    def l_yo(i, k):
        return pltpu.make_async_copy((xs, gs)[i].at[pl.ds(k * HALF, HALF), (lo, own_cols[0])[i]],
                                     (y_out, dx_out)[i].at[out_rows(k), :], loc.at[16 + 2 * i + k])

    stage = None
    for m, u in ((m, u) for u in range(8) for m in (1, 2)):
        b = buf[m, u, 0]
        if stage is None and b.shape != (2, ROWS, HALF):
            stage = [b.at[0], b.at[1]] if b.shape[0] == 2 else [b.at[0, pl.ds(k * SMALL, SMALL)] for k in (0, 1)]

    def finish(i, half):
        if half == 0:
            got(t_cp(i))
        acc, piece, dst = (yacc, dxacc)[i], (yl, dl)[i], (xs, gs)[i]

        def rows_of(q):
            return pl.ds(pl.multiple_of(half * HALF + q * SMALL, SMALL), SMALL)

        def fetch(q, k):
            return pltpu.make_async_copy(piece.at[rows_of(q), :], stage[k], isem.at[k])
        fetch(0, 0).start()

        def two(p, _):
            for k in (0, 1):
                q = 2 * p + k

                @pl.when(q + 1 < HALF // SMALL)
                def _():
                    fetch(q + 1, 1 - k).start()
                fetch(q, k).wait()
                rows = rows_of(q)
                dst[rows, :] = (acc[rows, :] + stage[k][...]).astype(BF16)
            return 0
        lax.fori_loop(0, HALF // SMALL // 2, two, 0)
        l_yo(i, half).start()

    def event(name):
        kind, a = name.rstrip("0123456789"), name.lstrip("abcdefghijklmnopqrstuvwxyz")
        n = int(a[0]) if a else 0
        hop_of = [int(q) for q in a[:3]] + [int(a[3]) if len(a) > 3 else None]
        if kind == "gwy":
            go(*wy(n))
        elif kind == "gwxo":
            go(*wx(n), *wp(n))
        elif kind == "gt":
            go(*ty(n), *tp(n))
            for cp in tl(n):
                cp.start()
        elif kind in ("gwxf", "gwzx", "gwz"):
            go(*{"gwxf": wxf, "gwzx": wzx, "gwz": wz}[kind](n))
        elif kind == "gh":
            go(*[q[0] for q in hop(*hop_of)])
        elif kind == "ga":
            go(*gives(n, int(a[1]), True))
        elif kind == "gyo":
            go(t_yo(n, int(a[1])))
        elif kind == "fw":
            got(*wy_in(n))
        elif kind == "fzx":
            got(*wx_in(n))
        elif kind == "fz":
            got(*(wz(n) if ROUTES[n] == "B" else wxf(n)))
        elif kind == "lw":
            if n % 2 == 0:
                s = n // 2
                got(*wzx(s), *(wxf(s) if ROUTES[s] == "B" else wz(s)), *wp(s))
            load_w(n, n % 2, True)
        elif kind == "ft":
            got(*ty(n))
            go(*tf(n))
            for cp in tl(n):
                cp.wait()
        elif kind == "fr":
            got(*tp(n), *tf(n))
        elif kind == "b":
            add_hop(*hop_of)
        elif kind == "cp":
            go(t_cp(0), t_cp(1))
            for i in (0, 1):
                for cp in tf(i):
                    cp.wait_send()
        elif kind == "fin":
            finish(n, int(a[1]))

    def zero(i, _):
        rows = pl.ds(pl.multiple_of(i * 64, 64), 64)
        yacc[rows, :] = jnp.zeros((64, HID), F32)
        dxacc[rows, :] = jnp.zeros((64, HID), F32)
        return 0
    plan = {n: list(v) for n, v in PLAN.items()}
    plan.setdefault(1, []).append("fr0")
    plan.setdefault(3, []).append("fr1")
    first = [q for q in range(len(plan[0])) if plan[0][q][0] != "g"][0]
    for name in plan[0][:first]:
        event(name)
    lax.fori_loop(0, TOK // 64, zero, 0)
    for name in plan[0][first:]:
        event(name)

    def tile(n, _):
        for at in sorted(plan):
            if 0 < at < NCH * NT:
                @pl.when(n == at)
                def _():
                    for name in plan[at]:
                        event(name)
        j, q = n // NT, n % NT
        slot = j % 2

        @pl.when(q == 0)
        def _():
            load_w(j, slot, False)
        w1, w2 = w1s.at[slot], w2s.at[slot]
        t = (q % 2) * 2 + q // 2
        rows = pl.ds(pl.multiple_of(t * TILE, TILE), TILE)
        xt, gt = xs[rows, :], gs[rows, :]
        u = dot(xt, w1[...], 1, 0)
        da = dot(gt, w2[...], 1, 1)
        cdf = 0.5 * (1.0 + lax.erf(u * INV_ROOT_TWO))
        act = (u * cdf).astype(BF16)
        du = (da * (cdf + u * jnp.exp(-0.5 * u * u) * INV_ROOT_TAU)).astype(BF16)
        yacc[rows, :] += dot(act, w2[...], 1, 0)
        dxacc[rows, :] += dot(du, w1[...], 1, 1)
        p2, p1 = dot(act, gt, 0, 0), dot(du, xt, 0, 0)

        @pl.when(q == 0)
        def _():
            d2[j] = p2
            d1[j] = p1

        @pl.when(q > 0)
        def _():
            d2[j] += p2
            d1[j] += p1
        return 0
    lax.fori_loop(0, NCH * NT, tile, 0)
    for name in plan[NCH * NT]:
        event(name)

    for s in range(4):
        for cp in wy(s) + wx(s) + wp(s) + wxf(s) + wzx(s) + wz(s):
            cp.wait_send()
    for m, u in ((m, u) for m in (1, 2) for u in range(8)):
        for h in range(3):
            for cp, _, _ in hop(m, u, h):
                cp.wait_send()
        for cp in gives(m, u, False) + gives(m, u, True):
            cp.wait_send()
            cp.wait_recv()
        for cp in stores(m, u):
            cp.wait()
    for i in (0, 1):
        for cp in ty(i) + tp(i) + [t_cp(i), t_yo(i, 0), t_yo(i, 1)]:
            cp.wait_send()
        for k in (0, 1):
            got(t_yo(i, k))
            l_yo(i, k).wait()


def fused(tok, grad, up, down):
    any_spec = pl.BlockSpec(memory_space=pl.ANY)
    vm, shape = pltpu.VMEM, jax.ShapeDtypeStruct
    land = [vm(dims, F32) for m in (1, 2) for u in range(8) for dims in hop_shapes(ORDERS[m][u])]
    dma = pltpu.SemaphoreType.DMA
    return pl.pallas_call(
        kernel,
        name="mlp_block",
        out_shape=(shape((TOK, HALF), BF16), shape((TOK, HALF), BF16), shape((2048, 256), F32), shape((1024, HALF), F32),
                   shape((TOK // 2, HID), F32), shape((TOK // 2, HID), F32),
                   shape((2, HID, HID), BF16), shape((2, HID, HID), BF16)),
        in_specs=[any_spec] * 4,
        out_specs=[any_spec] * 8,
        scratch_shapes=[
            vm((TOK, HID), BF16), vm((TOK, HID), BF16), vm((TOK, HID), F32), vm((TOK, HID), F32),
            vm((NCH, FC, HID), F32), vm((NCH, FC, HID), F32), vm((2, HID, FC), BF16), vm((2, FC, HID), BF16),
            dma((250,)), dma((250,)), dma((20,)), dma((2, 5)), dma((4,)), *land,
        ],
        compiler_params=pltpu.CompilerParams(collective_id=0, has_side_effects=True, vmem_limit_bytes=67_043_328),
    )(tok, grad, up, down)


def settle_kernel(y_in, dx_in, d1_in, d2_in, y_ref, dx_ref, d1_ref, d2_ref):
    y_ref[...] = y_in[...]
    dx_ref[...] = dx_in[...]
    d1_ref[...] = d1_in[...].T
    d2_ref[...] = d2_in[...]


def settle(y, dx, d1t, d2):
    steps = 2
    shape = jax.ShapeDtypeStruct

    def rows(n, cols):
        return pl.BlockSpec((n // steps, cols), lambda i: (i, 0))
    return pl.pallas_call(
        settle_kernel,
        name="settle",
        grid=(steps,),
        out_shape=(shape(y.shape, BF16), shape(dx.shape, BF16), shape(d1t.shape[::-1], F32), shape(d2.shape, F32)),
        in_specs=[rows(TOK, HALF), rows(TOK, HALF), rows(2048, 256), rows(1024, HALF)],
        out_specs=[rows(TOK, HALF), rows(TOK, HALF), pl.BlockSpec((256, 2048 // steps), lambda i: (0, i)), rows(1024, HALF)],
    )(y, dx, d1t, d2)


def solution(mesh):
    act_spec = P(("depth", "row"), "col")
    wgt_spec = P("row", "col")

    def block(tok, up, down, grad):
        return settle(*fused(tok, grad, up, down)[:4])

    return jax.shard_map(block, mesh=mesh, in_specs=(act_spec, wgt_spec, wgt_spec, act_spec),
                         out_specs=(act_spec, act_spec, wgt_spec, wgt_spec), check_vma=False)
```

```python
import math
import jax
import jax.numpy as jnp
from jax import lax
from jax.experimental import pallas as pl
from jax.experimental.pallas import tpu as pltpu
from jax.sharding import PartitionSpec as P

INV_ROOT_TWO = 1.0 / math.sqrt(2.0)
INV_ROOT_TAU = 1.0 / math.sqrt(2.0 * math.pi)
MESH = pl.DeviceIdType.MESH
BF16, F32 = jnp.bfloat16, jnp.float32

TOK, HID, FC, NCH = 2048, 1024, 256, 8
HALF, TILE, ROWS, SMALL = 512, 512, 128, 64
NT = TOK // TILE
GWY, GWXO, GT, GWXF, GWZX, GWZ, GH, GA, GYO, FW, FZX, FZ, LW, FT, FR, BH, CP, FIN = range(18)
ROUTES = "ABBA"
ORDERS = {1: ("CZB", "ZCB", "CBZ", "ZBC", "CZB", "ZCB", "ZBC", "CBZ"),
          2: ("CBZ", "CBZ", "BZC", "CBZ", "BCZ", "CBZ", "CBZ", "BZC")}
PLAN = {
    0: (110000, 10001, 110001, 10000, 110002, 210000, 1010000, 910001, 510001, 410000, 110003, 1010001,
        910000, 410001, 1110001, 310000, 1010002, 410002, 310001, 1010003, 410003, 210001, 1110000, 510000,
        1310000, 1210000, 1210001, 10002,),
    2: (10003, 1310001,),
    4: (910002, 1210002, 641000, 642100, 510002,),
    5: (641100,),
    6: (910003, 310003, 642000,),
    8: (1110002, 1210003, 1541000, 310002, 642101, 641101,),
    9: (1542100,),
    10: (1110003, 1541100, 642001, 510003,),
    11: (1542000,),
    12: (1541101, 641200, 642300,),
    13: (1542101,),
    14: (641001, 641300,),
    15: (1210004, 1542001,),
    16: (1210005, 642200, 642301, 641301,),
    17: (1541200, 1542300,),
    19: (1541001, 1541300, 630101,),
    20: (1210006, 1542301, 641201, 642500, 641500,),
    21: (1541301, 630131,),
    23: (1542200, 1530101, 641400, 630102, 630221,),
    24: (1210007, 1542500, 642501,),
    25: (641401, 641501,),
    26: (1541201, 1541500, 1530131, 630121,),
    27: (1530102, 642400, 720010,),
    28: (1541400, 1530221, 641600,),
    29: (1542501, 642600,),
    30: (1541401, 1541501, 630141,),
    31: (630222,),
    32: (1600000, 1530121, 641700, 642601, 630122, 1541600, 1542600, 642700, 1542400, 630241, 1530222,
        720022, 1530141, 641601, 630142, 1720000, 1541700, 1542601, 1720001, 1530122, 641701, 820000,
        1530241, 630242, 1720010, 1530142, 630201, 720014, 1720011, 1542700, 1541601, 630271, 630161,
        630261, 1541701, 1530242, 630171, 630151, 1530201, 630202, 820011, 1530271, 630211, 1530161,
        1530261, 630262, 1530202, 630162, 1530171, 630172, 1530151, 630132, 630272, 1530262, 630111,
        630152, 1530211, 630212, 820001, 1530162, 720016, 1530172, 630231, 1530132, 720013, 1530272,
        720027, 1530212, 1530152, 630251, 720015, 1530111, 630112, 820010, 1530231, 630232, 1530251,
        630252, 1530112, 720011, 1530232, 1530252,),
}

def dot(a, b, ca, cb):
    return lax.dot_general(a, b, (((ca,), (cb,)), ((), ())), preferred_element_type=F32)


def hop_shapes(order):
    nb, rows, cols, shapes = 2, ROWS, HID, []
    for h, kind in enumerate(order):
        if kind == "B":
            nb = 1
        elif kind == "C":
            cols = HALF
        elif h < 2:
            rows = ROWS // 2
        shapes.append((nb, rows, cols))
    return shapes


def kernel(x_in, g_in, up_in, down_in, y_out, dx_out, d1_out, d2_out, yl, dl, w1b, w2b,
           xs, gs, yacc, dxacc, d1, d2, w1s, w2s, send, recv, loc, wsem, isem, *land):
    z, y, r = lax.axis_index("depth"), lax.axis_index("col"), lax.axis_index("row")
    x, c = r // 2, r % 2
    r_x = (1 - x) * 2 + c
    r_c = r + 1 - 2 * c
    dev_c, dev_x, dev_xc = (z, y, r_c), (z, y, r_x), (z, y, (1 - x) * 2 + 1 - c)
    dev_y, dev_yc, dev_z, dev_zc = (z, 1 - y, r), (z, 1 - y, r_c), (1 - z, y, r), (1 - z, y, r_c)
    everything, lo, hi = slice(None), pl.ds(0, HALF), pl.ds(HALF, HALF)
    zrow = pl.ds(pl.multiple_of(z * ROWS, ROWS), ROWS)
    zoth = pl.ds(pl.multiple_of((1 - z) * ROWS, ROWS), ROWS)
    slots = {}

    def slot_of(name):
        return slots.setdefault(name, len(slots))

    def rc(name, src, dst, dev, arrives=None):
        return pltpu.make_async_remote_copy(
            src_ref=src, dst_ref=dst, send_sem=send.at[slot_of(name)],
            recv_sem=recv.at[slot_of(name if arrives is None else arrives)], device_id=dev, device_id_type=MESH)

    def go(*copies):
        for cp in copies:
            cp.start()

    def got(*copies):
        for cp in copies:
            cp.wait_recv()

    barrier = pltpu.get_barrier_semaphore()
    for dev in (dev_c, dev_x, dev_xc, dev_y, dev_yc, dev_z, dev_zc):
        pl.semaphore_signal(barrier, inc=1, device_id=dev, device_id_type=MESH)
    pl.semaphore_wait(barrier, 7)

    def chunk(q):
        return pl.ds(pl.multiple_of(q * FC, FC), FC)

    def up_cols(core, s):
        return pl.ds(pl.multiple_of(core * HID + s * FC, FC), FC)

    def part(xh, core, zi):
        return pl.ds(pl.multiple_of(xh * HALF + core * FC + zi * ROWS, ROWS), ROWS)

    def down_rows(s):
        return pl.ds(pl.multiple_of(s * FC + z * ROWS, ROWS), ROWS)

    def by_core(name, s, core, src, dst, dev):
        base = slot_of(f"{name}{s}0")
        slot_of(f"{name}{s}1")
        return pltpu.make_async_remote_copy(src_ref=src, dst_ref=dst, send_sem=send.at[base + core],
                                            recv_sem=recv.at[base + c], device_id=dev, device_id_type=MESH)

    def by_core_in(name, s, core, like):
        base = slot_of(f"{name}{s}0")
        slot_of(f"{name}{s}1")
        return pltpu.make_async_remote_copy(src_ref=like, dst_ref=like, send_sem=send.at[base + core],
                                            recv_sem=recv.at[base + core], device_id=dev_c, device_id_type=MESH)

    def wy(s):
        two = [by_core("wy", s, q, up_in.at[zrow, up_cols(q, s)], w1b.at[y, part(0, c, z), chunk(s)], (z, 1 - y, x * 2 + q))
               for q in (0, 1)]
        return two + [wy_down(s)]

    def wy_down(s):
        return rc(f"wY{s}", down_in.at[down_rows(s), :], w2b.at[x, down_rows(s), hi], dev_y)

    def wy_in(s):
        return [by_core_in("wy", s, q, w1b.at[1 - y, part(0, q, z), chunk(s)]) for q in (0, 1)] + [wy_down(s)]

    def wx(s):
        two = [by_core("wx", s, q, up_in.at[zrow, up_cols(q, s)], w1b.at[y, part(1, c, z), chunk(s)],
                       (z, y, (1 - x) * 2 + q)) for q in (0, 1)]
        return two + [wx_down(s)]

    def wx_down(s):
        return rc(f"wX{s}", down_in.at[down_rows(s), :], w2b.at[x, down_rows(s), lo], dev_x)

    def wx_in(s):
        return [by_core_in("wx", s, q, w1b.at[y, part(1, q, z), chunk(s)]) for q in (0, 1)] + [wx_down(s)]

    def wp(s):
        return [rc(f"wp{s}", up_in.at[:, up_cols(1 - c, s)], w1b.at[y, chunk(c), chunk(s)], dev_c)]

    def wxf(s):
        if ROUTES[s] == "B":
            both = w2b.at[x, chunk(s), hi]
            return [rc(f"wf{s}0", w1b.at[1 - y, lo, chunk(s)], w1b.at[1 - y, hi, chunk(s)], dev_x),
                    rc(f"wF{s}", both, both, dev_x)]
        two = [rc(f"wf{s}{q}", w1b.at[1 - y, part(0, q, z), chunk(s)], w1b.at[1 - y, part(1, q, z), chunk(s)], dev_x)
               for q in (0, 1)]
        both = w2b.at[x, down_rows(s), hi]
        return two + [rc(f"wF{s}", both, both, dev_x)]

    def same_z(name, ref):
        return rc(name, ref, ref, dev_z)

    def wzx(s):
        return [same_z(f"wzx{s}{q}", w1b.at[y, part(1, q, z), chunk(s)]) for q in (0, 1)] + [
            same_z(f"wzX{s}", w2b.at[1 - x, down_rows(s), lo])]

    def wz(s):
        if ROUTES[s] == "B":
            return [same_z(f"wz{s}0{q}", w1b.at[1 - y, part(0, q, z), chunk(s)]) for q in (0, 1)] + [
                same_z(f"wZ{s}0", w2b.at[x, down_rows(s), hi])]
        return [same_z(f"wz{s}{h}{q}", w1b.at[1 - y, part(h, q, z), chunk(s)]) for h in (0, 1) for q in (0, 1)] + [
            same_z(f"wZ{s}{i}", w2b.at[(x, 1 - x)[i], down_rows(s), hi]) for i in (0, 1)]

    def load_w(j, slot, start):
        s, b = j // 2, j % 2

        def cp(src, dst, k):
            copy = pltpu.make_async_copy(src, dst, wsem.at[slot, k])
            copy.start() if start else copy.wait()
        v1, v2 = w1s.at[slot], w2s.at[slot]
        if start:
            @pl.when(b == y)
            def _():
                cp(up_in.at[:, up_cols(c, s)], v1.at[chunk(c), :], 0)

            @pl.when(b != y)
            def _():
                cp(w1b.at[b, chunk(c), chunk(s)], v1.at[chunk(c), :], 0)

            @pl.when(b == x)
            def _():
                cp(down_in.at[chunk(s), :], v2.at[:, lo], 3)

            @pl.when(b != x)
            def _():
                cp(w2b.at[b, chunk(s), lo], v2.at[:, lo], 3)
        else:
            cp(up_in.at[:, up_cols(c, s)], v1.at[chunk(c), :], 0)
            cp(down_in.at[chunk(s), :], v2.at[:, lo], 3)
        cp(w1b.at[b, chunk(1 - c), chunk(s)], v1.at[chunk(1 - c), :], 1)
        cp(w1b.at[b, hi, chunk(s)], v1.at[hi, :], 2)
        cp(w2b.at[b, chunk(s), hi], v2.at[:, hi], 4)

    own_cols = (pl.ds(pl.multiple_of(jnp.where(x == y, 0, HALF), HALF), HALF), lo)
    far_cols = (pl.ds(pl.multiple_of(jnp.where(x == y, HALF, 0), HALF), HALF), hi)
    ins, tok = (x_in, g_in), (xs, gs)

    def tok_at(base, i):
        return pl.ds(pl.multiple_of(base * (TOK // 2) + i * TILE, TILE), TILE)

    def ty(i):
        return [rc(f"ty{i}{k}", ins[k].at[tok_at(1 - y, i), :], tok[k].at[tok_at(0, i), (own_cols[0], hi)[k]], dev_y)
                for k in (0, 1)]

    def tp(i):
        return [rc(f"tp{i}{k}", ins[k].at[tok_at(y, i), :], tok[k].at[tok_at(1, i), own_cols[k]], dev_c) for k in (0, 1)]

    def tf(i):
        return [rc(f"tf{i}{k}", tok[k].at[tok_at(0, i), far_cols[k]], tok[k].at[tok_at(1, i), far_cols[k]], dev_c)
                for k in (0, 1)]

    def tl(i):
        return [pltpu.make_async_copy(ins[k].at[tok_at(y, i), :], tok[k].at[tok_at(0, i), own_cols[k]],
                                      isem.at[2 * i + k]) for k in (0, 1)]

    parts = {1: d1, 2: d2}
    buf = {(m, u, h): land[(m - 1) * 24 + u * 3 + h] for m in (1, 2) for u in range(8) for h in range(3)}
    keep_block = {1: y, 2: x}
    dev_of = {(1, "C"): dev_x, (1, "B"): dev_y, (1, "Z"): dev_z, (2, "C"): dev_y, (2, "B"): dev_x, (2, "Z"): dev_z}

    def z_rows(u, zi):
        return pl.ds(pl.multiple_of(u % 2 * ROWS + zi * (ROWS // 2), ROWS // 2), ROWS // 2)

    def live(m, u, h):
        first = u // 2 * 2
        blocks, rows, cols = [first, first + 1], pl.ds(u % 2 * ROWS, ROWS), everything
        for kind in ORDERS[m][u][:h]:
            if kind == "B":
                blocks = [first + keep_block[m]]
            elif kind == "C":
                cols = lo
            else:
                rows = z_rows(u, z)
        return blocks, rows, cols

    def hop(m, u, h, only=None):
        kind = ORDERS[m][u][h]
        blocks, rows, cols = live(m, u, h)
        d, b, dev, first = parts[m], buf[m, u, h], dev_of[m, kind], u // 2 * 2
        if kind == "B":
            ends = [(d.at[first + 1 - keep_block[m], rows, cols], (first + keep_block[m], rows, cols))]
        elif kind == "C":
            ends = [(d.at[q, rows, hi], (q, rows, lo)) for q in blocks]
        elif h < 2:
            ends = [(d.at[q, z_rows(u, 1 - z), cols], (q, z_rows(u, z), cols)) for q in blocks]
        else:
            ends = [(d.at[q, rows, cols], (q, rows, cols)) for q in blocks]
        return [(rc(f"h{m}{u}{h}{i}", src, b.at[i], dev), b.at[i], into)
                for i, (src, into) in enumerate(ends) if only is None or i == only]

    def add_hop(m, s, h, only=None):
        for cp, landed, (q, rows, cols) in hop(m, s, h, only):
            got(cp)
            if h < 2:
                parts[m][q, rows, cols] += landed[...]
            else:
                landed[...] += parts[m][q, rows, cols]
        if h == 2:
            go(*gives(m, s, False))
            for cp in stores(m, s):
                cp.start()

    def fin_rows(m, u):
        split = ORDERS[m][u][2] != "Z"
        base = u * ROWS + (c * HID if m == 1 else 0)
        if split:
            base = base + z * (ROWS // 2)
        return pl.ds(pl.multiple_of(base, ROWS // 2), ROWS // 2 if split else ROWS)

    def cols_c(q):
        return pl.ds(pl.multiple_of(q * 256, 256), 256)

    def gives(m, s, far):
        b, split = buf[m, s, 2], ORDERS[m][s][2] != "Z"
        rows = fin_rows(m, s)
        if far and not split or m == 2 and not far:
            return []
        if m == 2:
            return [rc(f"a2{s}", b.at[0], d2_out.at[rows, :], dev_z)]
        if not far:
            return [rc(f"c1{s}", b.at[0, :, cols_c(1 - c)], d1_out.at[rows, :], dev_c)]
        return [rc(f"a1{s}", b.at[0, :, cols_c(c)], d1_out.at[rows, :], dev_z),
                rc(f"k1{s}", b.at[0, :, cols_c(1 - c)], d1_out.at[rows, :], dev_zc)]

    def stores(m, s):
        b = buf[m, s, 2]
        if m == 2:
            return [pltpu.make_async_copy(b.at[0], d2_out.at[fin_rows(m, s), :], loc.at[8 + s])]
        return [pltpu.make_async_copy(b.at[0, :, cols_c(c)], d1_out.at[fin_rows(m, s), :], loc.at[s])]

    mine, theirs = pl.ds(0, TOK // 2), pl.ds(TOK // 2, TOK // 2)

    def t_cp(i):
        return rc(f"cp{i}", (yacc, dxacc)[i].at[theirs, :], (yl, dl)[i], dev_c)

    def out_rows(k):
        return pl.ds(pl.multiple_of(y * (TOK // 2) + k * HALF, HALF), HALF)

    def t_yo(i, k):
        return rc(f"yo{i}{k}", (xs, gs)[i].at[pl.ds(k * HALF, HALF), (hi, far_cols[0])[i]],
                  (y_out, dx_out)[i].at[out_rows(k), :], dev_y)

    def l_yo(i, k):
        return pltpu.make_async_copy((xs, gs)[i].at[pl.ds(k * HALF, HALF), (lo, own_cols[0])[i]],
                                     (y_out, dx_out)[i].at[out_rows(k), :], loc.at[16 + 2 * i + k])

    stage = None
    for m, u in ((m, u) for u in range(8) for m in (1, 2)):
        b = buf[m, u, 0]
        if stage is None and b.shape != (2, ROWS, HALF):
            stage = [b.at[0], b.at[1]] if b.shape[0] == 2 else [b.at[0, pl.ds(k * SMALL, SMALL)] for k in (0, 1)]

    def finish(i, half):
        if half == 0:
            got(t_cp(i))
        acc, piece, dst = (yacc, dxacc)[i], (yl, dl)[i], (xs, gs)[i]

        def rows_of(q):
            return pl.ds(pl.multiple_of(half * HALF + q * SMALL, SMALL), SMALL)

        def fetch(q, k):
            return pltpu.make_async_copy(piece.at[rows_of(q), :], stage[k], isem.at[k])
        fetch(0, 0).start()

        def two(p, _):
            for k in (0, 1):
                q = 2 * p + k

                @pl.when(q + 1 < HALF // SMALL)
                def _():
                    fetch(q + 1, 1 - k).start()
                fetch(q, k).wait()
                rows = rows_of(q)
                dst[rows, :] = (acc[rows, :] + stage[k][...]).astype(BF16)
            return 0
        lax.fori_loop(0, HALF // SMALL // 2, two, 0)
        l_yo(i, half).start()

    def event(code):
        kind, count = code // 100000, code // 10000 % 10
        args = [code // 10**k % 10 for k in reversed(range(count))]
        n = args[0] if args else 0
        if kind == GWY:
            go(*wy(n))
        elif kind == GWXO:
            go(*wx(n), *wp(n))
        elif kind == GT:
            go(*ty(n), *tp(n))
            for cp in tl(n):
                cp.start()
        elif kind == GWXF:
            go(*wxf(n))
        elif kind == GWZX:
            go(*wzx(n))
        elif kind == GWZ:
            go(*wz(n))
        elif kind == GH:
            go(*[q[0] for q in hop(*args)])
        elif kind == GA:
            go(*gives(*args, True))
        elif kind == GYO:
            go(t_yo(*args))
        elif kind == FW:
            got(*wy_in(n))
        elif kind == FZX:
            got(*wx_in(n))
        elif kind == FZ:
            got(*(wz(n) if ROUTES[n] == "B" else wxf(n)))
        elif kind == LW:
            if n % 2 == 0:
                s = n // 2
                got(*wzx(s), *(wxf(s) if ROUTES[s] == "B" else wz(s)), *wp(s))
            load_w(n, n % 2, True)
        elif kind == FT:
            got(*ty(n))
            go(*tf(n))
            for cp in tl(n):
                cp.wait()
        elif kind == FR:
            got(*tp(n), *tf(n))
        elif kind == BH:
            add_hop(*args)
        elif kind == CP:
            go(t_cp(0), t_cp(1))
            for i in (0, 1):
                for cp in tf(i):
                    cp.wait_send()
        elif kind == FIN:
            finish(*args)

    def zero(i, _):
        rows = pl.ds(pl.multiple_of(i * 64, 64), 64)
        yacc[rows, :] = jnp.zeros((64, HID), F32)
        dxacc[rows, :] = jnp.zeros((64, HID), F32)
        return 0
    plan = {n: list(v) for n, v in PLAN.items()}
    plan.setdefault(1, []).append(FR * 100000 + 10000)
    plan.setdefault(3, []).append(FR * 100000 + 10001)
    first = [q for q in range(len(plan[0])) if plan[0][q] // 100000 > GYO][0]
    for name in plan[0][:first]:
        event(name)
    lax.fori_loop(0, TOK // 64, zero, 0)
    for name in plan[0][first:]:
        event(name)

    def tile(n, _):
        for at in sorted(plan):
            if 0 < at < NCH * NT:
                @pl.when(n == at)
                def _():
                    for name in plan[at]:
                        event(name)
        j, q = n // NT, n % NT
        slot = j % 2

        @pl.when(q == 0)
        def _():
            load_w(j, slot, False)
        w1, w2 = w1s.at[slot], w2s.at[slot]
        t = (q % 2) * 2 + q // 2
        rows = pl.ds(pl.multiple_of(t * TILE, TILE), TILE)
        xt, gt = xs[rows, :], gs[rows, :]
        u = dot(xt, w1[...], 1, 0)
        da = dot(gt, w2[...], 1, 1)
        cdf = 0.5 * (1.0 + lax.erf(u * INV_ROOT_TWO))
        act = (u * cdf).astype(BF16)
        du = (da * (cdf + u * jnp.exp(-0.5 * u * u) * INV_ROOT_TAU)).astype(BF16)
        yacc[rows, :] += dot(act, w2[...], 1, 0)
        dxacc[rows, :] += dot(du, w1[...], 1, 1)
        p2, p1 = dot(act, gt, 0, 0), dot(du, xt, 0, 0)

        @pl.when(q == 0)
        def _():
            d2[j] = p2
            d1[j] = p1

        @pl.when(q > 0)
        def _():
            d2[j] += p2
            d1[j] += p1
        return 0
    lax.fori_loop(0, NCH * NT, tile, 0)
    for name in plan[NCH * NT]:
        event(name)

    for s in range(4):
        for cp in wy(s) + wx(s) + wp(s) + wxf(s) + wzx(s) + wz(s):
            cp.wait_send()
    for m, u in ((m, u) for m in (1, 2) for u in range(8)):
        for h in range(3):
            for cp, _, _ in hop(m, u, h):
                cp.wait_send()
        for cp in gives(m, u, False) + gives(m, u, True):
            cp.wait_send()
            cp.wait_recv()
        for cp in stores(m, u):
            cp.wait()
    for i in (0, 1):
        for cp in ty(i) + tp(i) + [t_cp(i), t_yo(i, 0), t_yo(i, 1)]:
            cp.wait_send()
        for k in (0, 1):
            got(t_yo(i, k))
            l_yo(i, k).wait()


def fused(tok, grad, up, down):
    any_spec = pl.BlockSpec(memory_space=pl.ANY)
    vm, shape = pltpu.VMEM, jax.ShapeDtypeStruct
    land = [vm(dims, F32) for m in (1, 2) for u in range(8) for dims in hop_shapes(ORDERS[m][u])]
    dma = pltpu.SemaphoreType.DMA
    return pl.pallas_call(
        kernel,
        name="mlp_block",
        out_shape=(shape((TOK, HALF), BF16), shape((TOK, HALF), BF16), shape((2048, 256), F32), shape((1024, HALF), F32),
                   shape((TOK // 2, HID), F32), shape((TOK // 2, HID), F32),
                   shape((2, HID, HID), BF16), shape((2, HID, HID), BF16)),
        in_specs=[any_spec] * 4,
        out_specs=[any_spec] * 8,
        scratch_shapes=[
            vm((TOK, HID), BF16), vm((TOK, HID), BF16), vm((TOK, HID), F32), vm((TOK, HID), F32),
            vm((NCH, FC, HID), F32), vm((NCH, FC, HID), F32), vm((2, HID, FC), BF16), vm((2, FC, HID), BF16),
            dma((250,)), dma((250,)), dma((20,)), dma((2, 5)), dma((4,)), *land,
        ],
        compiler_params=pltpu.CompilerParams(collective_id=0, has_side_effects=True, vmem_limit_bytes=67_043_328),
    )(tok, grad, up, down)


def settle_kernel(y_in, dx_in, d1_in, d2_in, y_ref, dx_ref, d1_ref, d2_ref):
    y_ref[...] = y_in[...]
    dx_ref[...] = dx_in[...]
    d1_ref[...] = d1_in[...].T
    d2_ref[...] = d2_in[...]


def settle(y, dx, d1t, d2):
    steps = 2
    shape = jax.ShapeDtypeStruct

    def rows(n, cols):
        return pl.BlockSpec((n // steps, cols), lambda i: (i, 0))
    return pl.pallas_call(
        settle_kernel,
        name="settle",
        grid=(steps,),
        out_shape=(shape(y.shape, BF16), shape(dx.shape, BF16), shape(d1t.shape[::-1], F32), shape(d2.shape, F32)),
        in_specs=[rows(TOK, HALF), rows(TOK, HALF), rows(2048, 256), rows(1024, HALF)],
        out_specs=[rows(TOK, HALF), rows(TOK, HALF), pl.BlockSpec((256, 2048 // steps), lambda i: (0, i)), rows(1024, HALF)],
    )(y, dx, d1t, d2)


def solution(mesh):
    act_spec = P(("depth", "row"), "col")
    wgt_spec = P("row", "col")

    def block(tok, up, down, grad):
        return settle(*fused(tok, grad, up, down)[:4])

    return jax.shard_map(block, mesh=mesh, in_specs=(act_spec, wgt_spec, wgt_spec, act_spec),
                         out_specs=(act_spec, act_spec, wgt_spec, wgt_spec), check_vma=False)
```

```python
import math
import jax
import jax.numpy as jnp
from jax import lax
from jax.experimental import pallas as pl
from jax.experimental.pallas import tpu as pltpu
from jax.sharding import PartitionSpec as P

INV_ROOT_TWO = 1.0 / math.sqrt(2.0)
INV_ROOT_TAU = 1.0 / math.sqrt(2.0 * math.pi)
MESH = pl.DeviceIdType.MESH
BF16, F32 = jnp.bfloat16, jnp.float32

TOK, HID, FC, NCH = 2048, 1024, 256, 8
HALF, TILE, ROWS, SMALL = 512, 512, 128, 64
NT = TOK // TILE
GWY, GWXO, GT, GWXF, GWZX, GWZ, GH, GA, GYO, FW, FZX, FZ, LW, FT, FR, BH, CP, FIN = range(18)
ROUTES = "ABBA"
ORDERS = {1: ("CZB", "ZCB", "CBZ", "ZBC", "CZB", "ZCB", "ZBC", "CBZ"),
          2: ("CBZ", "CBZ", "BZC", "CBZ", "BCZ", "CBZ", "CBZ", "BZC")}
PLAN = (
    (110000, 10001, 110001, 10000, 110002, 210000, 1010000, 910001, 510001, 410000, 110003, 1010001, 910000,
     410001, 1110001, 310000, 1010002, 410002, 310001, 1010003, 410003, 210001, 1110000, 510000, 1310000,
     1210000, 1210001, 10002,),
    (),
    (10003, 1310001,),
    (),
    (910002, 1210002, 641000, 642100, 510002,),
    (641100,),
    (910003, 310003, 642000,),
    (),
    (1110002, 1210003, 1541000, 310002, 642101, 641101,),
    (1542100,),
    (1110003, 1541100, 642001, 510003,),
    (1542000,),
    (1541101, 641200, 642300,),
    (1542101,),
    (641001, 641300,),
    (1210004, 1542001,),
    (1210005, 642200, 642301, 641301,),
    (1541200, 1542300,),
    (),
    (1541001, 1541300, 630101,),
    (1210006, 1542301, 641201, 642500, 641500,),
    (1541301, 630131,),
    (),
    (1542200, 1530101, 641400, 630102, 630221,),
    (1210007, 1542500, 642501,),
    (641401, 641501,),
    (1541201, 1541500, 1530131, 630121,),
    (1530102, 642400, 720010,),
    (1541400, 1530221, 641600,),
    (1542501, 642600,),
    (1541401, 1541501, 630141,),
    (630222,),
    (1600000, 1530121, 641700, 642601, 630122, 1541600, 1542600, 642700, 1542400, 630241, 1530222, 720022,
     1530141, 641601, 630142, 1720000, 1541700, 1542601, 1720001, 1530122, 641701, 820000, 1530241, 630242,
     1720010, 1530142, 630201, 720014, 1720011, 1542700, 1541601, 630271, 630161, 630261, 1541701, 1530242,
     630171, 630151, 1530201, 630202, 820011, 1530271, 630211, 1530161, 1530261, 630262, 1530202, 630162,
     1530171, 630172, 1530151, 630132, 630272, 1530262, 630111, 630152, 1530211, 630212, 820001, 1530162,
     720016, 1530172, 630231, 1530132, 720013, 1530272, 720027, 1530212, 1530152, 630251, 720015, 1530111,
     630112, 820010, 1530231, 630232, 1530251, 630252, 1530112, 720011, 1530232, 1530252,),
)

def dot(a, b, ca, cb):
    return lax.dot_general(a, b, (((ca,), (cb,)), ((), ())), preferred_element_type=F32)


def hop_shapes(order):
    nb, rows, cols, shapes = 2, ROWS, HID, []
    for h, kind in enumerate(order):
        if kind == "B":
            nb = 1
        elif kind == "C":
            cols = HALF
        elif h < 2:
            rows = ROWS // 2
        shapes.append((nb, rows, cols))
    return shapes


def kernel(x_in, g_in, up_in, down_in, y_out, dx_out, d1_out, d2_out, yl, dl, w1b, w2b,
           xs, gs, yacc, dxacc, d1, d2, w1s, w2s, send, recv, loc, wsem, isem, *land):
    z, y, r = lax.axis_index("depth"), lax.axis_index("col"), lax.axis_index("row")
    x, c = r // 2, r % 2
    r_x = (1 - x) * 2 + c
    r_c = r + 1 - 2 * c
    dev_c, dev_x, dev_xc = (z, y, r_c), (z, y, r_x), (z, y, (1 - x) * 2 + 1 - c)
    dev_y, dev_yc, dev_z, dev_zc = (z, 1 - y, r), (z, 1 - y, r_c), (1 - z, y, r), (1 - z, y, r_c)
    everything, lo, hi = slice(None), pl.ds(0, HALF), pl.ds(HALF, HALF)
    zrow = pl.ds(pl.multiple_of(z * ROWS, ROWS), ROWS)
    zoth = pl.ds(pl.multiple_of((1 - z) * ROWS, ROWS), ROWS)
    slots = {}

    def slot_of(name):
        return slots.setdefault(name, len(slots))

    def rc(name, src, dst, dev, arrives=None):
        return pltpu.make_async_remote_copy(
            src_ref=src, dst_ref=dst, send_sem=send.at[slot_of(name)],
            recv_sem=recv.at[slot_of(name if arrives is None else arrives)], device_id=dev, device_id_type=MESH)

    def go(*copies):
        for cp in copies:
            cp.start()

    def got(*copies):
        for cp in copies:
            cp.wait_recv()

    barrier = pltpu.get_barrier_semaphore()
    for dev in (dev_c, dev_x, dev_xc, dev_y, dev_yc, dev_z, dev_zc):
        pl.semaphore_signal(barrier, inc=1, device_id=dev, device_id_type=MESH)
    pl.semaphore_wait(barrier, 7)

    def chunk(q):
        return pl.ds(pl.multiple_of(q * FC, FC), FC)

    def up_cols(core, s):
        return pl.ds(pl.multiple_of(core * HID + s * FC, FC), FC)

    def part(xh, core, zi):
        return pl.ds(pl.multiple_of(xh * HALF + core * FC + zi * ROWS, ROWS), ROWS)

    def down_rows(s):
        return pl.ds(pl.multiple_of(s * FC + z * ROWS, ROWS), ROWS)

    def by_core(name, s, core, src, dst, dev):
        base = slot_of(f"{name}{s}0")
        slot_of(f"{name}{s}1")
        return pltpu.make_async_remote_copy(src_ref=src, dst_ref=dst, send_sem=send.at[base + core],
                                            recv_sem=recv.at[base + c], device_id=dev, device_id_type=MESH)

    def by_core_in(name, s, core, like):
        base = slot_of(f"{name}{s}0")
        slot_of(f"{name}{s}1")
        return pltpu.make_async_remote_copy(src_ref=like, dst_ref=like, send_sem=send.at[base + core],
                                            recv_sem=recv.at[base + core], device_id=dev_c, device_id_type=MESH)

    def wy(s):
        two = [by_core("wy", s, q, up_in.at[zrow, up_cols(q, s)], w1b.at[y, part(0, c, z), chunk(s)], (z, 1 - y, x * 2 + q))
               for q in range(2)]
        return two + [wy_down(s)]

    def wy_down(s):
        return rc(f"wY{s}", down_in.at[down_rows(s), :], w2b.at[x, down_rows(s), hi], dev_y)

    def wy_in(s):
        return [by_core_in("wy", s, q, w1b.at[1 - y, part(0, q, z), chunk(s)]) for q in range(2)] + [wy_down(s)]

    def wx(s):
        two = [by_core("wx", s, q, up_in.at[zrow, up_cols(q, s)], w1b.at[y, part(1, c, z), chunk(s)],
                       (z, y, (1 - x) * 2 + q)) for q in range(2)]
        return two + [wx_down(s)]

    def wx_down(s):
        return rc(f"wX{s}", down_in.at[down_rows(s), :], w2b.at[x, down_rows(s), lo], dev_x)

    def wx_in(s):
        return [by_core_in("wx", s, q, w1b.at[y, part(1, q, z), chunk(s)]) for q in range(2)] + [wx_down(s)]

    def wp(s):
        return [rc(f"wp{s}", up_in.at[:, up_cols(1 - c, s)], w1b.at[y, chunk(c), chunk(s)], dev_c)]

    def wxf(s):
        if ROUTES[s] == "B":
            both = w2b.at[x, chunk(s), hi]
            return [rc(f"wf{s}0", w1b.at[1 - y, lo, chunk(s)], w1b.at[1 - y, hi, chunk(s)], dev_x),
                    rc(f"wF{s}", both, both, dev_x)]
        two = [rc(f"wf{s}{q}", w1b.at[1 - y, part(0, q, z), chunk(s)], w1b.at[1 - y, part(1, q, z), chunk(s)], dev_x)
               for q in range(2)]
        both = w2b.at[x, down_rows(s), hi]
        return two + [rc(f"wF{s}", both, both, dev_x)]

    def same_z(name, ref):
        return rc(name, ref, ref, dev_z)

    def wzx(s):
        return [same_z(f"wzx{s}{q}", w1b.at[y, part(1, q, z), chunk(s)]) for q in range(2)] + [
            same_z(f"wzX{s}", w2b.at[1 - x, down_rows(s), lo])]

    def wz(s):
        if ROUTES[s] == "B":
            return [same_z(f"wz{s}0{q}", w1b.at[1 - y, part(0, q, z), chunk(s)]) for q in range(2)] + [
                same_z(f"wZ{s}0", w2b.at[x, down_rows(s), hi])]
        return [same_z(f"wz{s}{h}{q}", w1b.at[1 - y, part(h, q, z), chunk(s)]) for h in range(2) for q in range(2)] + [
            same_z(f"wZ{s}{i}", w2b.at[(x, 1 - x)[i], down_rows(s), hi]) for i in range(2)]

    def load_w(j, slot, start):
        s, b = j // 2, j % 2

        def cp(src, dst, k):
            copy = pltpu.make_async_copy(src, dst, wsem.at[slot, k])
            copy.start() if start else copy.wait()
        v1, v2 = w1s.at[slot], w2s.at[slot]
        if start:
            @pl.when(b == y)
            def _():
                cp(up_in.at[:, up_cols(c, s)], v1.at[chunk(c), :], 0)

            @pl.when(b != y)
            def _():
                cp(w1b.at[b, chunk(c), chunk(s)], v1.at[chunk(c), :], 0)

            @pl.when(b == x)
            def _():
                cp(down_in.at[chunk(s), :], v2.at[:, lo], 3)

            @pl.when(b != x)
            def _():
                cp(w2b.at[b, chunk(s), lo], v2.at[:, lo], 3)
        else:
            cp(up_in.at[:, up_cols(c, s)], v1.at[chunk(c), :], 0)
            cp(down_in.at[chunk(s), :], v2.at[:, lo], 3)
        cp(w1b.at[b, chunk(1 - c), chunk(s)], v1.at[chunk(1 - c), :], 1)
        cp(w1b.at[b, hi, chunk(s)], v1.at[hi, :], 2)
        cp(w2b.at[b, chunk(s), hi], v2.at[:, hi], 4)

    own_cols = (pl.ds(pl.multiple_of(jnp.where(x == y, 0, HALF), HALF), HALF), lo)
    far_cols = (pl.ds(pl.multiple_of(jnp.where(x == y, HALF, 0), HALF), HALF), hi)
    ins, tok = (x_in, g_in), (xs, gs)

    def tok_at(base, i):
        return pl.ds(pl.multiple_of(base * (TOK // 2) + i * TILE, TILE), TILE)

    def ty(i):
        return [rc(f"ty{i}{k}", ins[k].at[tok_at(1 - y, i), :], tok[k].at[tok_at(0, i), (own_cols[0], hi)[k]], dev_y)
                for k in range(2)]

    def tp(i):
        return [rc(f"tp{i}{k}", ins[k].at[tok_at(y, i), :], tok[k].at[tok_at(1, i), own_cols[k]], dev_c) for k in range(2)]

    def tf(i):
        return [rc(f"tf{i}{k}", tok[k].at[tok_at(0, i), far_cols[k]], tok[k].at[tok_at(1, i), far_cols[k]], dev_c)
                for k in range(2)]

    def tl(i):
        return [pltpu.make_async_copy(ins[k].at[tok_at(y, i), :], tok[k].at[tok_at(0, i), own_cols[k]],
                                      isem.at[2 * i + k]) for k in range(2)]

    parts = {1: d1, 2: d2}
    buf = {(m, u, h): land[(m - 1) * 24 + u * 3 + h] for m in (1, 2) for u in range(8) for h in range(3)}
    keep_block = {1: y, 2: x}
    dev_of = {(1, "C"): dev_x, (1, "B"): dev_y, (1, "Z"): dev_z, (2, "C"): dev_y, (2, "B"): dev_x, (2, "Z"): dev_z}

    def z_rows(u, zi):
        return pl.ds(pl.multiple_of(u % 2 * ROWS + zi * (ROWS // 2), ROWS // 2), ROWS // 2)

    def live(m, u, h):
        first = u // 2 * 2
        blocks, rows, cols = [first, first + 1], pl.ds(u % 2 * ROWS, ROWS), everything
        for kind in ORDERS[m][u][:h]:
            if kind == "B":
                blocks = [first + keep_block[m]]
            elif kind == "C":
                cols = lo
            else:
                rows = z_rows(u, z)
        return blocks, rows, cols

    def hop(m, u, h, only=None):
        kind = ORDERS[m][u][h]
        blocks, rows, cols = live(m, u, h)
        d, b, dev, first = parts[m], buf[m, u, h], dev_of[m, kind], u // 2 * 2
        if kind == "B":
            ends = [(d.at[first + 1 - keep_block[m], rows, cols], (first + keep_block[m], rows, cols))]
        elif kind == "C":
            ends = [(d.at[q, rows, hi], (q, rows, lo)) for q in blocks]
        elif h < 2:
            ends = [(d.at[q, z_rows(u, 1 - z), cols], (q, z_rows(u, z), cols)) for q in blocks]
        else:
            ends = [(d.at[q, rows, cols], (q, rows, cols)) for q in blocks]
        return [(rc(f"h{m}{u}{h}{i}", src, b.at[i], dev), b.at[i], into)
                for i, (src, into) in enumerate(ends) if only is None or i == only]

    def add_hop(m, s, h, only=None):
        for cp, landed, (q, rows, cols) in hop(m, s, h, only):
            got(cp)
            if h < 2:
                parts[m][q, rows, cols] += landed[...]
            else:
                landed[...] += parts[m][q, rows, cols]
        if h == 2:
            go(*gives(m, s, False))
            for cp in stores(m, s):
                cp.start()

    def fin_rows(m, u):
        split = ORDERS[m][u][2] != "Z"
        base = u * ROWS + (c * HID if m == 1 else 0)
        if split:
            base = base + z * (ROWS // 2)
        return pl.ds(pl.multiple_of(base, ROWS // 2), ROWS // 2 if split else ROWS)

    def cols_c(q):
        return pl.ds(pl.multiple_of(q * 256, 256), 256)

    def gives(m, s, far):
        b, split = buf[m, s, 2], ORDERS[m][s][2] != "Z"
        rows = fin_rows(m, s)
        if far and not split or m == 2 and not far:
            return []
        if m == 2:
            return [rc(f"a2{s}", b.at[0], d2_out.at[rows, :], dev_z)]
        if not far:
            return [rc(f"c1{s}", b.at[0, :, cols_c(1 - c)], d1_out.at[rows, :], dev_c)]
        return [rc(f"a1{s}", b.at[0, :, cols_c(c)], d1_out.at[rows, :], dev_z),
                rc(f"k1{s}", b.at[0, :, cols_c(1 - c)], d1_out.at[rows, :], dev_zc)]

    def stores(m, s):
        b = buf[m, s, 2]
        if m == 2:
            return [pltpu.make_async_copy(b.at[0], d2_out.at[fin_rows(m, s), :], loc.at[8 + s])]
        return [pltpu.make_async_copy(b.at[0, :, cols_c(c)], d1_out.at[fin_rows(m, s), :], loc.at[s])]

    mine, theirs = pl.ds(0, TOK // 2), pl.ds(TOK // 2, TOK // 2)

    def t_cp(i):
        return rc(f"cp{i}", (yacc, dxacc)[i].at[theirs, :], (yl, dl)[i], dev_c)

    def out_rows(k):
        return pl.ds(pl.multiple_of(y * (TOK // 2) + k * HALF, HALF), HALF)

    def t_yo(i, k):
        return rc(f"yo{i}{k}", (xs, gs)[i].at[pl.ds(k * HALF, HALF), (hi, far_cols[0])[i]],
                  (y_out, dx_out)[i].at[out_rows(k), :], dev_y)

    def l_yo(i, k):
        return pltpu.make_async_copy((xs, gs)[i].at[pl.ds(k * HALF, HALF), (lo, own_cols[0])[i]],
                                     (y_out, dx_out)[i].at[out_rows(k), :], loc.at[16 + 2 * i + k])

    stage = None
    for m, u in ((m, u) for u in range(8) for m in (1, 2)):
        b = buf[m, u, 0]
        if stage is None and b.shape != (2, ROWS, HALF):
            stage = [b.at[0], b.at[1]] if b.shape[0] == 2 else [b.at[0, pl.ds(k * SMALL, SMALL)] for k in range(2)]

    def finish(i, half):
        if half == 0:
            got(t_cp(i))
        acc, piece, dst = (yacc, dxacc)[i], (yl, dl)[i], (xs, gs)[i]

        def rows_of(q):
            return pl.ds(pl.multiple_of(half * HALF + q * SMALL, SMALL), SMALL)

        def fetch(q, k):
            return pltpu.make_async_copy(piece.at[rows_of(q), :], stage[k], isem.at[k])
        fetch(0, 0).start()

        def two(p, _):
            for k in range(2):
                q = 2 * p + k

                @pl.when(q + 1 < HALF // SMALL)
                def _():
                    fetch(q + 1, 1 - k).start()
                fetch(q, k).wait()
                rows = rows_of(q)
                dst[rows, :] = (acc[rows, :] + stage[k][...]).astype(BF16)
            return 0
        lax.fori_loop(0, HALF // SMALL // 2, two, 0)
        l_yo(i, half).start()

    def event(code):
        kind, count = code // 100000, code // 10000 % 10
        args = [code // 10**k % 10 for k in reversed(range(count))]
        n = args[0] if args else 0
        if kind == GWY:
            go(*wy(n))
        elif kind == GWXO:
            go(*wx(n), *wp(n))
        elif kind == GT:
            go(*ty(n), *tp(n))
            for cp in tl(n):
                cp.start()
        elif kind == GWXF:
            go(*wxf(n))
        elif kind == GWZX:
            go(*wzx(n))
        elif kind == GWZ:
            go(*wz(n))
        elif kind == GH:
            go(*[q[0] for q in hop(*args)])
        elif kind == GA:
            go(*gives(*args, True))
        elif kind == GYO:
            go(t_yo(*args))
        elif kind == FW:
            got(*wy_in(n))
        elif kind == FZX:
            got(*wx_in(n))
        elif kind == FZ:
            got(*(wz(n) if ROUTES[n] == "B" else wxf(n)))
        elif kind == LW:
            if n % 2 == 0:
                s = n // 2
                got(*wzx(s), *(wxf(s) if ROUTES[s] == "B" else wz(s)), *wp(s))
            load_w(n, n % 2, True)
        elif kind == FT:
            got(*ty(n))
            go(*tf(n))
            for cp in tl(n):
                cp.wait()
        elif kind == FR:
            got(*tp(n), *tf(n))
        elif kind == BH:
            add_hop(*args)
        elif kind == CP:
            go(t_cp(0), t_cp(1))
            for i in range(2):
                for cp in tf(i):
                    cp.wait_send()
        elif kind == FIN:
            finish(*args)

    def zero(i, _):
        rows = pl.ds(pl.multiple_of(i * 64, 64), 64)
        yacc[rows, :] = jnp.zeros((64, HID), F32)
        dxacc[rows, :] = jnp.zeros((64, HID), F32)
        return 0
    plan = [list(v) for v in PLAN]
    plan[1].append(FR * 100000 + 10000)
    plan[3].append(FR * 100000 + 10001)
    first = [q for q in range(len(plan[0])) if plan[0][q] // 100000 > GYO][0]
    for name in plan[0][:first]:
        event(name)
    lax.fori_loop(0, TOK // 64, zero, 0)
    for name in plan[0][first:]:
        event(name)

    def tile(n, _):
        for at in range(1, NCH * NT):
            if plan[at]:
                @pl.when(n == at)
                def _():
                    for name in plan[at]:
                        event(name)
        j, q = n // NT, n % NT
        slot = j % 2

        @pl.when(q == 0)
        def _():
            load_w(j, slot, False)
        w1, w2 = w1s.at[slot], w2s.at[slot]
        t = (q % 2) * 2 + q // 2
        rows = pl.ds(pl.multiple_of(t * TILE, TILE), TILE)
        xt, gt = xs[rows, :], gs[rows, :]
        u = dot(xt, w1[...], 1, 0)
        da = dot(gt, w2[...], 1, 1)
        cdf = 0.5 * (1.0 + lax.erf(u * INV_ROOT_TWO))
        act = (u * cdf).astype(BF16)
        du = (da * (cdf + u * jnp.exp(-0.5 * u * u) * INV_ROOT_TAU)).astype(BF16)
        yacc[rows, :] += dot(act, w2[...], 1, 0)
        dxacc[rows, :] += dot(du, w1[...], 1, 1)
        p2, p1 = dot(act, gt, 0, 0), dot(du, xt, 0, 0)

        @pl.when(q == 0)
        def _():
            d2[j] = p2
            d1[j] = p1

        @pl.when(q > 0)
        def _():
            d2[j] += p2
            d1[j] += p1
        return 0
    lax.fori_loop(0, NCH * NT, tile, 0)
    for name in plan[NCH * NT]:
        event(name)

    for s in range(4):
        for cp in wy(s) + wx(s) + wp(s) + wxf(s) + wzx(s) + wz(s):
            cp.wait_send()
    for m, u in ((m, u) for m in (1, 2) for u in range(8)):
        for h in range(3):
            for cp, _, _ in hop(m, u, h):
                cp.wait_send()
        for cp in gives(m, u, False) + gives(m, u, True):
            cp.wait_send()
            cp.wait_recv()
        for cp in stores(m, u):
            cp.wait()
    for i in range(2):
        for cp in ty(i) + tp(i) + [t_cp(i), t_yo(i, 0), t_yo(i, 1)]:
            cp.wait_send()
        for k in range(2):
            got(t_yo(i, k))
            l_yo(i, k).wait()


def fused(tok, grad, up, down):
    any_spec = pl.BlockSpec(memory_space=pl.ANY)
    vm, shape = pltpu.VMEM, jax.ShapeDtypeStruct
    land = [vm(dims, F32) for m in (1, 2) for u in range(8) for dims in hop_shapes(ORDERS[m][u])]
    dma = pltpu.SemaphoreType.DMA
    return pl.pallas_call(
        kernel,
        name="mlp_block",
        out_shape=(shape((TOK, HALF), BF16), shape((TOK, HALF), BF16), shape((2048, 256), F32), shape((1024, HALF), F32),
                   shape((TOK // 2, HID), F32), shape((TOK // 2, HID), F32),
                   shape((2, HID, HID), BF16), shape((2, HID, HID), BF16)),
        in_specs=[any_spec] * 4,
        out_specs=[any_spec] * 8,
        scratch_shapes=[
            vm((TOK, HID), BF16), vm((TOK, HID), BF16), vm((TOK, HID), F32), vm((TOK, HID), F32),
            vm((NCH, FC, HID), F32), vm((NCH, FC, HID), F32), vm((2, HID, FC), BF16), vm((2, FC, HID), BF16),
            dma((250,)), dma((250,)), dma((20,)), dma((2, 5)), dma((4,)), *land,
        ],
        compiler_params=pltpu.CompilerParams(collective_id=0, has_side_effects=True, vmem_limit_bytes=67_043_328),
    )(tok, grad, up, down)


def settle_kernel(y_in, dx_in, d1_in, d2_in, y_ref, dx_ref, d1_ref, d2_ref):
    y_ref[...] = y_in[...]
    dx_ref[...] = dx_in[...]
    d1_ref[...] = d1_in[...].T
    d2_ref[...] = d2_in[...]


def settle(y, dx, d1t, d2):
    steps = 2
    shape = jax.ShapeDtypeStruct

    def rows(n, cols):
        return pl.BlockSpec((n // steps, cols), lambda i: (i, 0))
    return pl.pallas_call(
        settle_kernel,
        name="settle",
        grid=(steps,),
        out_shape=(shape(y.shape, BF16), shape(dx.shape, BF16), shape(d1t.shape[::-1], F32), shape(d2.shape, F32)),
        in_specs=[rows(TOK, HALF), rows(TOK, HALF), rows(2048, 256), rows(1024, HALF)],
        out_specs=[rows(TOK, HALF), rows(TOK, HALF), pl.BlockSpec((256, 2048 // steps), lambda i: (0, i)), rows(1024, HALF)],
    )(y, dx, d1t, d2)


def solution(mesh):
    act_spec = P(("depth", "row"), "col")
    wgt_spec = P("row", "col")

    def block(tok, up, down, grad):
        return settle(*fused(tok, grad, up, down)[:4])

    return jax.shard_map(block, mesh=mesh, in_specs=(act_spec, wgt_spec, wgt_spec, act_spec),
                         out_specs=(act_spec, act_spec, wgt_spec, wgt_spec), check_vma=False)
```
